128 devices in a mesh: dp: 1, tp2: 16 (over z, y), tp: 8 (over x, core).
Axes of the slice: x: 4, y: 4, z: 4, core: 2. Of those that a mesh axis runs over, the one named last changes fastest.
Arguments:
- attn_out: bfloat16 [32768, 4096], P('dp', 'tp')
- w_out: bfloat16 [4096, 4096], P('tp', 'tp2')
- residual: bfloat16 [32768, 4096], P(('dp', 'tp'), 'tp2')
- norm_gain: float32 [4096], P('tp2')
Outputs:
- output 1: bfloat16 [32768, 4096], P(('dp', 'tp'), 'tp2')
- output 2: bfloat16 [32768, 4096], P(('dp', 'tp'), 'tp2')
All inputs are finite; a program needn't handle non-finite values.
Results may differ from the reference program's by a relative error of at most 0.00634374.
Values are sent between devices in bfloat16 or wider.
A program may use at most 1 GiB of HBM per device.

```python
import jax
import jax.numpy as jnp
from jax import lax

TOKENS = 32768
D = 4096
HEADS = 32
HEAD = 128
TP = 8
EPS_NORM = 1e-6


def setup_inputs(seed: int = 0, part: int = 0) -> dict:
    attn_width = HEADS * HEAD
    root_key = jax.random.key(seed)
    key_attn, key_w, key_res, key_gain = jax.random.split(root_key, 4)
    attn_vals = jax.random.normal(jax.random.fold_in(key_attn, part), (TOKENS, attn_width), jnp.float32)
    w_vals = jax.random.normal(key_w, (attn_width, D), jnp.float32) * (attn_width ** -0.5)
    res_vals = jax.random.normal(jax.random.fold_in(key_res, part), (TOKENS, D), jnp.float32)
    gain_vals = 1.0 + 0.3 * jax.random.normal(key_gain, (D,), jnp.float32)
    return {"attn_out": attn_vals.astype(jnp.bfloat16), "w_out": w_vals.astype(jnp.bfloat16), "residual": res_vals.astype(jnp.bfloat16), "norm_gain": gain_vals}


def reference(attn_out, w_out, residual, norm_gain):
    attn_width = attn_out.shape[1]
    shard_cols = attn_width // TP
    attn_shards = attn_out.reshape(TOKENS, TP, shard_cols).transpose(1, 0, 2)
    w_shards = w_out.reshape(TP, shard_cols, D)

    def add_shard(running, shard_pair):
        attn_blk, w_blk = shard_pair
        block_prod = jnp.dot(attn_blk, w_blk, preferred_element_type=jnp.float32).astype(jnp.bfloat16)
        return running + block_prod.astype(jnp.float32), None

    y_sum, _ = lax.scan(add_shard, jnp.zeros((TOKENS, D), jnp.float32), (attn_shards, w_shards))
    hidden = residual.astype(jnp.float32) + y_sum
    mean_sq = jnp.mean(hidden * hidden, axis=-1, keepdims=True)
    normed = hidden * lax.rsqrt(mean_sq + EPS_NORM) * norm_gain
    return hidden.astype(jnp.bfloat16), normed.astype(jnp.bfloat16)
```

```python
import jax
import jax.numpy as jnp
from jax import lax
from jax.experimental import pallas as pl
from jax.experimental.pallas import tpu as pltpu
from jax.sharding import PartitionSpec as P

EPS_NORM = 1e-6
MESH = pl.DeviceIdType.MESH
BF16, F32 = jnp.bfloat16, jnp.float32

NC = 8
CR = 128
SUB = 32
KB = 512
CB = 256
WZ = 256


def kernel(a_hbm, w_hbm, r_hbm, g_ref, h_hbm, n_hbm,
           abuf, wbuf, yout, yin, rbuf, hbuf, nbuf, sq,
           l_sem, a_s, a_r, p_s, p_r, b_s, b_r, f_s, f_r, w_s, w_r, d_s, d_r, y_s, y_r, q_s, q_r, o_s):
    tp, t2 = lax.axis_index("tp"), lax.axis_index("tp2")
    x, c, z, y = tp // 2, tp % 2, t2 // 4, t2 % 4

    def dev(dx=0, dy=0, dz=0, core=None):
        return {"tp": ((x + dx) % 4) * 2 + (c if core is None else core), "tp2": ((z + dz) % 4) * 4 + (y + dy) % 4}

    def rdma(src, dst, ssem, rsem, device):
        return pltpu.make_async_remote_copy(src_ref=src, dst_ref=dst, send_sem=ssem, recv_sem=rsem,
                                            device_id=device, device_id_type=MESH)

    ym, yp = (y + 3) % 4, (y + 1) % 4

    def cross(k, d, cd):
        block = (((x + d) % 4) * 2 + cd) * (4 * NC) + z * NC + k
        return rdma(a_hbm.at[block, y], abuf.at[k, y, c, (4 - d) % 4], a_s.at[k, d - 1, cd], a_r.at[k, c],
                    dev(dx=d, core=cd))

    def cross_wait(k, cc):
        view = abuf.at[k, y, cc, pl.ds(1, 3)]
        pltpu.make_async_copy(view, view, a_r.at[k, cc]).wait()

    def bcast(k, cc, back):
        view = abuf.at[k, y, cc, pl.ds(1, 3)]
        return rdma(view, view, b_s.at[k, cc, back], b_r.at[k, cc, back], dev(dy=3 if back else 1))

    def forward(k, back):
        view = abuf.at[k, yp if back else ym, back, pl.ds(1, 3)]
        return rdma(view, view, f_s.at[k, back], f_r.at[k, back], dev(dy=3 if back else 1))

    def ysend(k, zr):
        return rdma(yout.at[k, zr - 1], yin.at[z * NC + k], y_s.at[k, zr - 1], y_r.at[k, zr - 1], dev(dz=zr))

    def wview(part, j, zr):
        return wbuf.at[j, c, zr, pl.ds(0, WZ) if part == 0 else pl.ds(WZ, KB - WZ)]

    w_sends = []

    def wsend(part, src_slot, dst_slot, device):
        n = len(w_sends)
        copy = rdma(wview(part, *src_slot), wview(part, *dst_slot), w_s.at[n],
                    w_r.at[part, dst_slot[0] * 4 + dst_slot[1]], device)
        w_sends.append(copy)
        copy.start()

    def wwait(part, slot):
        view = wview(part, *slot)
        pltpu.make_async_copy(view, view, w_r.at[part, slot[0] * 4 + slot[1]]).wait()

    def dcopy(part, slot):
        view = wview(part, *slot)
        n = slot[0] * 4 + slot[1]
        return rdma(view, view, d_s.at[part, n], d_r.at[part, n], dev(core=1 - c))

    own_a = pltpu.make_async_copy(a_hbm.at[pl.ds(tp * (4 * NC) + z * NC, NC)], abuf.at[:, :, c, 0], l_sem.at[0])
    own_w = pltpu.make_async_copy(w_hbm, wbuf.at[0, c, 0], l_sem.at[1])
    own_r = pltpu.make_async_copy(r_hbm, rbuf, l_sem.at[2])
    own_w.start()
    own_a.start()
    own_r.start()

    barrier = pltpu.get_barrier_semaphore()
    peers = [dev(dx=d, core=cd) for d in (1, 2, 3) for cd in (0, 1)] + [dev(core=1 - c)]
    peers += [dev(dy=1), dev(dy=3), dev(dz=1), dev(dz=2), dev(dz=3)]
    for peer in peers:
        pl.semaphore_signal(barrier, inc=1, device_id=peer, device_id_type=MESH)
    pl.semaphore_wait(barrier, len(peers))

    def cross_start(k):
        for d in (1, 3, 2):
            for cd in (0, 1):
                cross(k, d, cd).start()

    partner_a = rdma(a_hbm.at[pl.ds((tp + 1 - 2 * c) * (4 * NC) + z * NC, NC)], abuf.at[:, :, c, 0],
                     p_s, p_r, dev(core=1 - c))
    cross_start(0)
    own_w.wait()
    for zr, dz in ((3, 1), (1, 3), (2, 2)):
        wsend(0, (0, 0), (0, zr), dev(dz=dz))
    for j, dx in ((3, 1), (1, 3), (2, 2)):
        wsend(1, (0, 0), (j, 0), dev(dx=dx))
    cross_start(1)
    partner_a.start()
    dcopy(0, (0, 0)).start()
    dcopy(1, (0, 0)).start()

    def bcast_start(k):
        for cc in (0, 1):
            cross_wait(k, cc)
        for i in (0, 1):
            bcast(k, i, 0).start()
            bcast(k, 1 - i, 1).start()

    def forward_start(k):
        for back in (0, 1):
            bcast(k, back, back).wait_recv()
            forward(k, back).start()

    bcast_start(0)

    for zr in (3, 1, 2, 0):
        if zr:
            wwait(0, (0, zr))
            dcopy(0, (0, zr)).start()
        wsend(0, (0, zr), (3, zr), dev(dx=1))
        wsend(0, (0, zr), (1, zr), dev(dx=3))
    for j in (0, 3, 1, 2):
        if j:
            wwait(1, (j, 0))
            dcopy(1, (j, 0)).start()
        wsend(1, (j, 0), (j, 3), dev(dz=1))
        wsend(1, (j, 0), (j, 1), dev(dz=3))
    cross_start(2)
    bcast_start(1)
    forward_start(0)

    for i in (0, 1):
        for j, zr, dx in ((3, (3, 1)[i], 1), (1, (2, 0)[i], 3)):
            wwait(0, (j, zr))
            wsend(0, (j, zr), (2, zr), dev(dx=dx))
            dcopy(0, (j, zr)).start()
        for zr, j, dz in ((3, (0, 3)[i], 1), (1, (1, 2)[i], 3)):
            wwait(1, (j, zr))
            wsend(1, (j, zr), (j, 2), dev(dz=dz))
            dcopy(1, (j, zr)).start()
    for k in range(3, NC):
        cross_start(k)
    for slot in ((3, 2), (3, 0), (1, 3), (1, 1)):
        wwait(0, slot)
        dcopy(0, slot).start()
    for slot in ((1, 3), (2, 3), (0, 1), (3, 1)):
        wwait(1, slot)
        dcopy(1, slot).start()
    for n in range(4):
        wwait(0, (2, n))
        dcopy(0, (2, n)).start()
        wwait(1, (n, 2))
        dcopy(1, (n, 2)).start()
    own_a.wait()
    partner_a.wait_recv()
    for n in range(16):
        for part in (0, 1):
            dcopy(part, (n // 4, n % 4)).wait_recv()

    def tile(k, zr, out):
        for j in range(4):
            for cc in (0, 1):
                lhs = abuf[k, :, cc, j].reshape(CR, KB)
                term = jnp.dot(lhs, wbuf[j, cc, zr], preferred_element_type=F32).astype(BF16).astype(F32)
                if j == 0 and cc == 0:
                    out[...] = term
                else:
                    out[...] += term

    def step(k, carry):
        @pl.when(k < NC - 2)
        def _():
            bcast_start(k + 2)

        @pl.when(k < NC - 1)
        def _():
            forward_start(k + 1)

        for back in (0, 1):
            bcast(k, 1 - back, back).wait_recv()
            forward(k, back).wait_recv()
        for zr in (1, 3, 2):
            tile(k, zr, yout.at[k, zr - 1])
            ysend(k, zr).start()
        tile(k, 0, yin.at[z * NC + k])
        return carry

    lax.fori_loop(0, NC, step, 0)

    own_r.wait()

    def qsend(g, n):
        view = sq.at[g, t2]
        return rdma(view, view, q_s.at[g, n - 1], q_r.at[g], dev(dy=n % 4, dz=n // 4))

    def square_group(g):
        for i in (0, 1):
            k = 2 * g + i
            for zr in (1, 2, 3):
                ysend(k, zr).wait_recv()
            for q in range(4):
                hid = yin[q * NC + k] + rbuf[q, pl.ds(k * CR, CR), :].astype(F32)
                yin[q * NC + k] = hid
                hbuf[q, pl.ds(k * CR, CR), :] = hid.astype(BF16)
                total = jnp.sum(hid * hid, axis=1, keepdims=True)
                sq[g, t2, pl.ds(i * 4 + q, 1), :] = jnp.broadcast_to(total, (CR, 128)).T[0:1, :]
        for n in range(1, 16):
            qsend(g, n).start()
        out_copy(hbuf, h_hbm, g, 0).start()

    def out_copy(buf, dst, g, which):
        rows = pl.ds(g * (2 * CR), 2 * CR)
        return pltpu.make_async_copy(buf.at[:, rows], dst.at[:, rows], o_s.at[g, which])

    def norm_group(g):
        view = sq.at[g, pl.ds(0, 15)]
        pltpu.make_async_copy(view, view, q_r.at[g]).wait()
        inv = lax.rsqrt(jnp.sum(sq[g], axis=0) * (1.0 / 4096) + EPS_NORM)
        for i in (0, 1):
            k = 2 * g + i
            for q in range(4):
                scale = jnp.broadcast_to(inv[i * 4 + q:i * 4 + q + 1, :], (128, CR)).T
                for half in (0, 1):
                    cols = pl.ds(half * 128, 128)
                    nbuf[q, pl.ds(k * CR, CR), cols] = (
                        yin[q * NC + k, :, cols] * scale * g_ref[:, cols]).astype(BF16)
        out_copy(nbuf, n_hbm, g, 1).start()

    groups = NC // 2

    def finish(g, carry):
        @pl.when(g < groups)
        def _():
            square_group(g)

        @pl.when(g >= 1)
        def _():
            norm_group(g - 1)

        return carry

    lax.fori_loop(0, groups + 1, finish, 0)

    for copy in w_sends:
        copy.wait_send()
    partner_a.wait_send()
    for n in range(16):
        for part in (0, 1):
            dcopy(part, (n // 4, n % 4)).wait_send()

    def drain(k, carry):
        for d in (1, 2, 3):
            for cd in (0, 1):
                cross(k, d, cd).wait_send()
            ysend(k, d).wait_send()
        for back in (0, 1):
            bcast(k, 0, back).wait_send()
            bcast(k, 1, back).wait_send()
            forward(k, back).wait_send()
        return carry

    lax.fori_loop(0, NC, drain, 0)

    def drain_group(g, carry):
        for n in range(1, 16):
            qsend(g, n).wait_send()
        out_copy(hbuf, h_hbm, g, 0).wait()
        out_copy(nbuf, n_hbm, g, 1).wait()
        return carry

    lax.fori_loop(0, groups, drain_group, 0)


def solution(mesh):
    def local_step(attn_blk, w_blk, res_blk, gain_blk):
        any_spec = pl.BlockSpec(memory_space=pl.ANY)
        out = jax.ShapeDtypeStruct((4, NC * CR, CB), BF16)
        dma = pltpu.SemaphoreType.DMA
        h, n = pl.pallas_call(
            kernel,
            out_shape=(out, out),
            in_specs=[any_spec, any_spec, any_spec, pl.BlockSpec(memory_space=pltpu.VMEM)],
            out_specs=(any_spec, any_spec),
            scratch_shapes=[
                pltpu.VMEM((NC, 4, 2, 4, SUB, KB), BF16),
                pltpu.VMEM((4, 2, 4, KB, CB), BF16),
                pltpu.VMEM((NC, 3, CR, CB), F32),
                pltpu.VMEM((4 * NC, CR, CB), F32),
                pltpu.VMEM((4, NC * CR, CB), BF16),
                pltpu.VMEM((4, NC * CR, CB), BF16),
                pltpu.VMEM((4, NC * CR, CB), BF16),
                pltpu.VMEM((NC // 2, 16, 8, 128), F32),
                dma((3,)),
                dma((NC, 3, 2)), dma((NC, 2)),
                dma, dma,
                dma((NC, 2, 2)), dma((NC, 2, 2)),
                dma((NC, 2)), dma((NC, 2)),
                dma((30,)), dma((2, 16)),
                dma((2, 16)), dma((2, 16)),
                dma((NC, 3)), dma((NC, 3)),
                dma((NC // 2, 15)), dma((NC // 2,)),
                dma((NC // 2, 2)),
            ],
            compiler_params=pltpu.CompilerParams(
                collective_id=0, has_side_effects=True, vmem_limit_bytes=60 * 1024 * 1024),
        )(attn_blk.reshape(8 * 4 * NC, 4, SUB, KB), w_blk, res_blk.reshape(4, NC * CR, CB), gain_blk.reshape(1, CB))
        return h.reshape(4 * NC * CR, CB), n.reshape(4 * NC * CR, CB)

    row_spec = P(("dp", "tp"), "tp2")
    return jax.shard_map(local_step, mesh=mesh, in_specs=(P("dp", "tp"), P("tp", "tp2"), row_spec, P("tp2")),
                         out_specs=(row_spec, row_spec), check_vma=False)
```

```python
import jax
import jax.numpy as jnp
from jax import lax
from jax.experimental import pallas as pl
from jax.experimental.pallas import tpu as pltpu
from jax.sharding import PartitionSpec as P

EPS_NORM = 1e-6
MESH = pl.DeviceIdType.MESH
AROUND = (1, 3, 2)
CORES = (0, 1)
BF16, F32 = jnp.bfloat16, jnp.float32

NC = 8
NK = 7
CR = 128
SUB = 32
KB = 512
CB = 256
WZ = 256


def kernel(a_hbm, w_hbm, r_hbm, yin, inv_ref,
           abuf, wbuf, yout, rbuf, sq, ea, eout, ein,
           l_sem, a_s, a_r, p_s, p_r, b_s, b_r, f_s, f_r, w_s, w_r, d_s, d_r, y_s, y_r, q_s, q_r, e_s, e_r):
    tp, t2 = lax.axis_index("tp"), lax.axis_index("tp2")
    x, c, z, y = tp // 2, tp % 2, t2 // 4, t2 % 4

    def dev(dx=0, dy=0, dz=0, core=None):
        return {"tp": ((x + dx) % 4) * 2 + (c if core is None else core), "tp2": ((z + dz) % 4) * 4 + (y + dy) % 4}

    def rdma(src, dst, ssem, rsem, device):
        return pltpu.make_async_remote_copy(src_ref=src, dst_ref=dst, send_sem=ssem, recv_sem=rsem,
                                            device_id=device, device_id_type=MESH)

    ym, yp = (y + 3) % 4, (y + 1) % 4

    def cross(k, d, cd):
        return rdma(a_hbm.at[(((x + d) % 4) * 2 + cd) * 4 + z, k, y], abuf.at[k, y, c, (4 - d) % 4], a_s.at[k, d - 1, cd], a_r.at[k, c],
                    dev(dx=d, core=cd))

    def cross_wait(k, cc):
        view = abuf.at[k, y, cc, pl.ds(1, 3)]
        pltpu.make_async_copy(view, view, a_r.at[k, cc]).wait()

    def bcast(k, cc, back):
        view = abuf.at[k, y, cc, pl.ds(1, 3)]
        return rdma(view, view, b_s.at[k, cc, back], b_r.at[k, cc, back], dev(dy=3 if back else 1))

    def forward(k, back):
        view = abuf.at[k, yp if back else ym, back, pl.ds(1, 3)]
        return rdma(view, view, f_s.at[k, back], f_r.at[k, back], dev(dy=3 if back else 1))

    def ysend(k, zr):
        return rdma(yout.at[k, zr - 1], yin.at[z * NC + k], y_s.at[k, zr - 1], y_r.at[k, zr - 1], dev(dz=zr))

    def wview(part, j, zr):
        return wbuf.at[j, c, zr, pl.ds(0, WZ) if part == 0 else pl.ds(WZ, KB - WZ)]

    w_sent = []

    def wcopy(n, part, src_slot, dst_slot, device):
        return rdma(wview(part, *src_slot), wview(part, *dst_slot), w_s.at[n],
                    w_r.at[part, dst_slot[0] * 4 + dst_slot[1]], device)

    def wsend(part, src_slot, dst_slot, device):
        wcopy(len(w_sent), part, src_slot, dst_slot, device).start()
        w_sent.append(part)

    def wwait(part, slot):
        view = wview(part, *slot)
        pltpu.make_async_copy(view, view, w_r.at[part, slot[0] * 4 + slot[1]]).wait()

    def dcopy(part, slot):
        view = wview(part, *slot)
        n = slot[0] * 4 + slot[1]
        return rdma(view, view, d_s.at[part, n], d_r.at[part, n], dev(core=1 - c))

    own_a = pltpu.make_async_copy(a_hbm.at[tp * 4 + z, pl.ds(0, NK)], abuf.at[:, :, c, 0], l_sem.at[0])
    ex_a = pltpu.make_async_copy(a_hbm.at[:, NK], ea, l_sem.at[3])
    own_w = pltpu.make_async_copy(w_hbm, wbuf.at[0, c, 0], l_sem.at[1])
    own_r = pltpu.make_async_copy(r_hbm, rbuf, l_sem.at[2])
    own_w.start()
    ex_a.start()
    own_a.start()
    own_r.start()

    barrier = pltpu.get_barrier_semaphore()
    peers = [dev(dx=d, core=cd) for d in AROUND for cd in CORES] + [dev(core=1 - c)]
    peers += [dev(dy=1), dev(dy=3), dev(dz=1), dev(dz=2), dev(dz=3)]
    for peer in peers:
        pl.semaphore_signal(barrier, inc=1, device_id=peer, device_id_type=MESH)
    pl.semaphore_wait(barrier, len(peers))

    def cross_start(k):
        for d in AROUND:
            for cd in CORES:
                cross(k, d, cd).start()

    def bcast_start(k):
        for cc in CORES:
            cross_wait(k, cc)
        for i in CORES:
            bcast(k, i, 0).start()
            bcast(k, 1 - i, 1).start()

    def forward_start(k):
        for back in CORES:
            bcast(k, back, back).wait_recv()
            forward(k, back).start()

    def take(part, j, zr):
        wwait(part, (j, zr))
        dcopy(part, (j, zr)).start()

    def relay_x(part, j, zr):
        take(part, j, zr)
        wsend(part, (j, zr), (2, zr), dev(dx=4 - j))

    def relay_z(j, zr):
        take(1, j, zr)
        wsend(1, (j, zr), (j, 2), dev(dz=4 - zr))

    def both_x(part, zr):
        wsend(part, (0, zr), (3, zr), dev(dx=1))
        wsend(part, (0, zr), (1, zr), dev(dx=3))

    def both_z(part, j):
        wsend(part, (j, 0), (j, 3), dev(dz=1))
        wsend(part, (j, 0), (j, 1), dev(dz=3))

    partner_a = rdma(a_hbm.at[(tp + 1 - 2 * c) * 4 + z, pl.ds(0, NK)], abuf.at[:, :, c, 0],
                     p_s, p_r, dev(core=1 - c))
    own_w.wait()
    wsend(0, (0, 0), (0, 3), dev(dz=1))
    wsend(0, (0, 0), (0, 1), dev(dz=3))
    cross_start(0)
    both_z(1, 0)
    both_x(1, 0)
    wsend(1, (0, 0), (2, 0), dev(dx=2))
    wsend(0, (0, 0), (0, 2), dev(dz=2))
    cross_start(1)
    cross_start(2)
    partner_a.start()
    dcopy(0, (0, 0)).start()
    dcopy(1, (0, 0)).start()

    ex_a.wait()

    def ex_copy(d, cd):
        owner = ((x + d) % 4) * 2 + cd
        return rdma(eout.at[owner], ein.at[tp], e_s.at[d, cd], e_r.at[tp], dev(dx=d, core=cd))

    def ex_product(i, carry):
        lhs = ea[pl.ds(i * 4, 4)].reshape(4 * CR, KB)
        prod = jnp.dot(lhs, wbuf[0, c, 0], preferred_element_type=F32)
        eout[i] = prod.astype(BF16).reshape(4, CR, CB)
        return carry

    lax.fori_loop(0, 8, ex_product, 0)

    take(0, 0, 3)
    take(0, 0, 1)
    wsend(0, (0, 3), (3, 3), dev(dx=1))
    wsend(0, (0, 1), (1, 1), dev(dx=3))
    wsend(0, (0, 1), (3, 1), dev(dx=1))
    wsend(0, (0, 3), (1, 3), dev(dx=3))
    bcast_start(0)
    for j in (3, 1, 2):
        take(1, j, 0)
        both_z(1, j)
    forward_start(0)
    relay_z(0, 3)
    take(1, 0, 1)
    take(0, 0, 2)
    bcast_start(1)
    bcast_start(2)
    relay_z(1, 1)
    relay_z(3, 3)
    forward_start(1)
    relay_x(0, 3, 3)
    relay_x(0, 1, 1)
    cross_start(3)
    both_x(0, 2)
    cross_start(4)
    relay_z(2, 1)
    for slot in ((3, 1), (1, 3), (2, 3)):
        take(1, *slot)
    take(0, 3, 1)
    take(0, 1, 3)
    take(0, 2, 3)
    take(0, 2, 1)
    own_a.wait()
    partner_a.wait_recv()

    def partner_w(zr):
        for j in range(4):
            for part in CORES:
                dcopy(part, (j, zr)).wait_recv()

    partner_w(1)
    partner_w(3)

    def tile(k, zr, out):
        for j in range(4):
            for cc in CORES:
                lhs = abuf[k, :, cc, j].reshape(CR, KB)
                term = jnp.dot(lhs, wbuf[j, cc, zr], preferred_element_type=F32).astype(BF16).astype(F32)
                if j == 0 and cc == 0:
                    out[...] = term
                else:
                    out[...] += term

    def qsend(g, n):
        view = sq.at[g, t2]
        return rdma(view, view, q_s.at[g, n - 1], q_r.at[g], dev(dy=n % 4, dz=n // 4))

    def square_group(g):
        for i in CORES:
            k = 2 * g + i
            if k < NK:
                for zr in AROUND:
                    ysend(k, zr).wait_recv()
            for q in range(4):
                hid = yin[q * NC + k] + rbuf[q, pl.ds(k * CR, CR), :].astype(F32)
                yin[q * NC + k] = hid
                total = jnp.sum(hid * hid, axis=1, keepdims=True)
                sq[g, t2, pl.ds(i * 4 + q, 1), :] = jnp.broadcast_to(total, (CR, 128)).T[0:1, :]
        for n in range(1, 16):
            qsend(g, n).start()

    def norm_group(g):
        view = sq.at[g, pl.ds(0, 15)]
        pltpu.make_async_copy(view, view, q_r.at[g]).wait()
        inv_ref[g] = lax.rsqrt(jnp.sum(sq[g], axis=0) * (1.0 / 4096) + EPS_NORM)

    def step(k, carry):
        for back in CORES:
            bcast(k, 1 - back, back).wait_recv()
            forward(k, back).wait_recv()
        for zr in (1, 3):
            tile(k, zr, yout.at[k, zr - 1])
            ysend(k, zr).start()

        @pl.when(k == 0)
        def _():
            forward_start(2)
            bcast_start(3)

        @pl.when(k == 1)
        def _():
            relay_x(0, 3, 2)
            for n in range(5, NK):
                cross_start(n)
            both_x(0, 0)
            take(0, 1, 2)
            for j in range(4):
                take(1, j, 2)

        @pl.when(k == 2)
        def _():
            forward_start(3)
            bcast_start(4)
            take(0, 2, 2)
            partner_w(2)
            bcast_start(5)

        @pl.when(k == 3)
        def _():
            forward_start(4)
            bcast_start(6)
            ex_copy(0, 1 - c).start()
            for d in AROUND:
                ex_copy(d, 0).start()

        @pl.when(k == 4)
        def _():
            forward_start(5)

        def far(i, carry):
            tile(i, 2, yout.at[i, 1])
            ysend(i, 2).start()
            return carry

        lax.fori_loop(jnp.where(k == 2, 0, k), jnp.where(k < 2, 0, k + 1), far, 0)

        @pl.when(k == 4)
        def _():
            relay_x(0, 3, 0)
            take(0, 1, 0)
            for d in AROUND:
                ex_copy(d, 1).start()
            forward_start(6)

        return carry

    own_r.wait()
    lax.fori_loop(0, NK, step, 0)
    take(0, 2, 0)
    partner_w(0)

    def near(i, carry):
        tile(i, 0, yin.at[z * NC + i])
        return carry

    lax.fori_loop(0, NK, near, 0)

    def ex_arrival(i):
        return pltpu.make_async_copy(ein.at[i], ein.at[i], e_r.at[i])

    for i in range(8):
        @pl.when(tp != i)
        def _():
            ex_arrival(i).wait()

    def ex_sum(q, carry):
        total = eout[tp, q].astype(F32)
        for d in range(1, 8):
            total += ein[(tp + d) % 8, q].astype(F32)
        yin[q * NC + NK] = total
        return carry

    lax.fori_loop(0, 4, ex_sum, 0)
    for g in range(NC // 2):
        square_group(g)
    for g in range(NC // 2):
        norm_group(g)

    for n, part in enumerate(w_sent):
        wcopy(n, part, (0, 0), (1, 0), dev(dx=1)).wait_send()
    partner_a.wait_send()
    for n in range(16):
        for part in CORES:
            dcopy(part, (n // 4, n % 4)).wait_send()

    def drain(k, carry):
        for d in AROUND:
            for cd in CORES:
                cross(k, d, cd).wait_send()
            ysend(k, d).wait_send()
        for back in CORES:
            bcast(k, 0, back).wait_send()
            bcast(k, 1, back).wait_send()
            forward(k, back).wait_send()
        return carry

    lax.fori_loop(0, NK, drain, 0)
    ex_copy(0, 1 - c).wait_send()
    for d in AROUND:
        ex_copy(d, 0).wait_send()
        ex_copy(d, 1).wait_send()

    def drain_group(g, carry):
        for n in range(1, 16):
            qsend(g, n).wait_send()
        return carry

    lax.fori_loop(0, NC // 2, drain_group, 0)


def norm_kernel(yin, inv_ref, g_ref, h_hbm, n_hbm, hbuf, nbuf, sem):
    def out_copy(k, which):
        rows = pl.ds(k * CR, CR)
        buf, dst = ((hbuf, h_hbm), (nbuf, n_hbm))[which]
        return pltpu.make_async_copy(buf.at[:, rows], dst.at[:, rows], sem.at[k, which])

    def chunk(k, carry):
        rows = pl.ds(k * CR, CR)
        for q in range(4):
            inv = inv_ref[k // 2, pl.ds((k % 2) * 4 + q, 1), :]
            scale = jnp.broadcast_to(inv, (128, CR)).T
            hid = yin[q * NC + k]
            hbuf[q, rows, :] = hid.astype(BF16)
            for half in CORES:
                cols = slice(half * 128, half * 128 + 128)
                nbuf[q, rows, cols] = (hid[:, cols] * scale * g_ref[:, cols]).astype(BF16)
        out_copy(k, 0).start()
        out_copy(k, 1).start()
        return carry

    lax.fori_loop(0, NC, chunk, 0)

    def drain(k, carry):
        out_copy(k, 0).wait()
        out_copy(k, 1).wait()
        return carry

    lax.fori_loop(0, NC, drain, 0)


def solution(mesh):
    def local_step(attn_blk, w_blk, res_blk, gain_blk):
        any_spec = pl.BlockSpec(memory_space=pl.ANY)
        out = jax.ShapeDtypeStruct((4, NC * CR, CB), BF16)
        vmem_spec = pl.BlockSpec(memory_space=pltpu.VMEM)
        dma = pltpu.SemaphoreType.DMA
        hidden, inv = pl.pallas_call(
            kernel,
            out_shape=(pltpu.VMEM((4 * NC, CR, CB), F32), pltpu.VMEM((NC // 2, 8, 128), F32)),
            in_specs=[any_spec, any_spec, any_spec],
            out_specs=(vmem_spec, vmem_spec),
            scratch_shapes=[
                pltpu.VMEM((NK, 4, 2, 4, SUB, KB), BF16),
                pltpu.VMEM((4, 2, 4, KB, CB), BF16),
                pltpu.VMEM((NK, 3, CR, CB), F32),
                pltpu.VMEM((4, NC * CR, CB), BF16),
                pltpu.VMEM((NC // 2, 16, 8, 128), F32),
                pltpu.VMEM((32, 4, SUB, KB), BF16),
                pltpu.VMEM((8, 4, CR, CB), BF16),
                pltpu.VMEM((8, 4, CR, CB), BF16),
                dma((4,)),
                dma((NK, 3, 2)), dma((NK, 2)),
                dma, dma,
                dma((NK, 2, 2)), dma((NK, 2, 2)),
                dma((NK, 2)), dma((NK, 2)),
                dma((30,)), dma((2, 16)),
                dma((2, 16)), dma((2, 16)),
                dma((NK, 3)), dma((NK, 3)),
                dma((NC // 2, 15)), dma((NC // 2,)),
                dma((4, 2)), dma((8,)),
            ],
            compiler_params=pltpu.CompilerParams(
                collective_id=0, has_side_effects=True, vmem_limit_bytes=50 * 1024 * 1024),
        )(attn_blk.reshape(8 * 4, NC, 4, SUB, KB), w_blk, res_blk.reshape(4, NC * CR, CB))
        h, n = pl.pallas_call(
            norm_kernel,
            out_shape=(out, out),
            in_specs=[vmem_spec] * 3,
            out_specs=(any_spec, any_spec),
            scratch_shapes=[pltpu.VMEM((4, NC * CR, CB), BF16)] * 2 + [dma((NC, 2))],
            compiler_params=pltpu.CompilerParams(vmem_limit_bytes=12 * 1024 * 1024),
        )(hidden, inv, gain_blk.reshape(1, CB))
        return h.reshape(4 * NC * CR, CB), n.reshape(4 * NC * CR, CB)

    row_spec = P(("dp", "tp"), "tp2")
    return jax.shard_map(local_step, mesh=mesh, in_specs=(P("dp", "tp"), P("tp", "tp2"), row_spec, P("tp2")),
                         out_specs=(row_spec, row_spec), check_vma=False)
```

```python
import jax
import jax.numpy as jnp
from jax import lax
from jax.experimental import pallas as pl
from jax.experimental.pallas import tpu as pltpu
from jax.sharding import PartitionSpec as P

EPS_NORM = 1e-6
MESH = pl.DeviceIdType.MESH
AROUND = (1, 3, 2)
CORES = (0, 1)
BF16, F32 = jnp.bfloat16, jnp.float32

NC = 8
NK = 7
CR = 128
LAST = NC // 2 - 1
SUB = 32
KB = 512
CB = 256
PARTS = ((0, 256), (256, 256), (256, 128), (384, 128))
HALVES = {3: 2, 1: 3}


def kernel(a_hbm, w_hbm, r_hbm, yin, inv_ref,
           abuf, wbuf, yout, rbuf, sq, sz, ea, eout, ein,
           l_sem, a_s, a_r, p_s, p_r, b_r, f_r, w_s, w_r, d_s, d_r, y_s, y_r, q_s, q_r, e_s, e_r, z_r):
    tp, t2 = lax.axis_index("tp"), lax.axis_index("tp2")
    x, c, z, y = tp // 2, tp % 2, t2 // 4, t2 % 4

    def dev(dx=0, dy=0, dz=0, core=None):
        return {"tp": ((x + dx) % 4) * 2 + (c if core is None else core), "tp2": ((z + dz) % 4) * 4 + (y + dy) % 4}

    def rdma(src, dst, ssem, rsem, device):
        return pltpu.make_async_remote_copy(src_ref=src, dst_ref=dst, send_sem=ssem, recv_sem=rsem,
                                            device_id=device, device_id_type=MESH)

    def await_bytes(view, sem):
        pltpu.make_async_copy(view, view, sem).wait()

    ym, yp = (y + 3) % 4, (y + 1) % 4

    def cross(k, d, cd):
        return rdma(a_hbm.at[(((x + d) % 4) * 2 + cd) * 4 + z, k, y], abuf.at[k, y, c, (4 - d) % 4], a_s, a_r.at[k],
                    dev(dx=d, core=cd))

    def bcast(k, cc, back):
        view = abuf.at[k, y, cc, pl.ds(1, 3)]
        return rdma(view, view, a_s, b_r.at[k, back] if cc == back else f_r.at[k], dev(dy=3 if back else 1))

    def forward(k, back):
        view = abuf.at[k, yp if back else ym, back, pl.ds(1, 3)]
        return rdma(view, view, a_s, f_r.at[k], dev(dy=3 if back else 1))

    def ysend(k, zr):
        return rdma(yout.at[k, zr - 1], yin.at[z * NC + k], y_s, y_r.at[k], dev(dz=zr))

    def wview(part, j, zr):
        return wbuf.at[j, c, zr, pl.ds(*PARTS[part])]

    def w_arrival(part, slot):
        return w_r.at[part % 2, 0 if part > 1 else slot[0] * 4 + slot[1]]

    def wsend(part, src_slot, dst_slot, device):
        rdma(wview(part, *src_slot), wview(part, *dst_slot), w_s, w_arrival(part, dst_slot), device).start()

    def dcopy(part, slot):
        view = wview(part, *slot)
        return rdma(view, view, d_s, d_r.at[slot[1]], dev(core=1 - c))

    own_a = pltpu.make_async_copy(a_hbm.at[tp * 4 + z, pl.ds(0, NK)], abuf.at[:, :, c, 0], l_sem.at[0])
    ex_a = pltpu.make_async_copy(a_hbm.at[:, NK], ea, l_sem.at[3])
    own_w = pltpu.make_async_copy(w_hbm, wbuf.at[0, c, 0], l_sem.at[1])
    own_r = pltpu.make_async_copy(r_hbm, rbuf, l_sem.at[2])
    own_w.start()
    ex_a.start()
    own_a.start()
    own_r.start()

    barrier = pltpu.get_barrier_semaphore()
    peers = [dev(dx=d, core=cd) for d in AROUND for cd in CORES] + [dev(core=1 - c)]
    peers += [dev(dy=1), dev(dy=3), dev(dz=1), dev(dz=2), dev(dz=3)]
    for peer in peers:
        pl.semaphore_signal(barrier, inc=1, device_id=peer, device_id_type=MESH)
    pl.semaphore_wait(barrier, len(peers))

    def cross_start(k):
        for d in AROUND:
            for cd in CORES:
                cross(k, d, cd).start()

    def bcast_start(k):
        await_bytes(abuf.at[k, y, :, pl.ds(1, 3)], a_r.at[k])
        for i in CORES:
            bcast(k, i, 0).start()
            bcast(k, 1 - i, 1).start()

    def forward_start(k):
        for back in CORES:
            bcast(k, back, back).wait_recv()
            forward(k, back).start()

    def take(part, j, zr):
        await_bytes(wview(part, j, zr), w_arrival(part, (j, zr)))
        dcopy(part, (j, zr)).start()

    def relay_x(part, j, zr):
        take(part, j, zr)
        wsend(part, (j, zr), (2, zr), dev(dx=4 - j))

    def relay_z(j, zr):
        take(1, j, zr)
        wsend(1, (j, zr), (j, 2), dev(dz=4 - zr))

    def both_x(part, zr):
        wsend(part, (0, zr), (3, zr), dev(dx=1))
        wsend(part, (0, zr), (1, zr), dev(dx=3))

    def both_z(part, j):
        wsend(part, (j, 0), (j, 3), dev(dz=1))
        wsend(part, (j, 0), (j, 1), dev(dz=3))

    partner_a = rdma(a_hbm.at[(tp + 1 - 2 * c) * 4 + z, pl.ds(0, NK)], abuf.at[:, :, c, 0],
                     p_s, p_r, dev(core=1 - c))
    own_w.wait()
    wsend(0, (0, 0), (0, 3), dev(dz=1))
    wsend(0, (0, 0), (0, 1), dev(dz=3))
    cross_start(0)
    both_z(1, 0)
    both_x(1, 0)
    wsend(0, (0, 0), (0, 2), dev(dz=2))
    cross_start(1)
    partner_a.start()
    dcopy(0, (0, 0)).start()
    dcopy(1, (0, 0)).start()

    ex_a.wait()

    def ex_copy(d, cd):
        owner = ((x + d) % 4) * 2 + cd
        return rdma(eout.at[owner], ein.at[tp], e_s, e_r, dev(dx=d, core=cd))

    def ex_product(i, carry):
        lhs = ea[pl.ds(i * 4, 4)].reshape(4 * CR, KB)
        prod = jnp.dot(lhs, wbuf[0, c, 0], preferred_element_type=F32)
        eout[i] = prod.astype(BF16).reshape(4, CR, CB)
        return carry

    lax.fori_loop(0, 8, ex_product, 0)

    take(0, 0, 3)
    take(0, 0, 1)
    wsend(0, (0, 3), (3, 3), dev(dx=1))
    wsend(0, (0, 1), (1, 1), dev(dx=3))
    wsend(0, (0, 1), (3, 1), dev(dx=1))
    wsend(0, (0, 3), (1, 3), dev(dx=3))
    bcast_start(0)
    for j, half in HALVES.items():
        take(1, j, 0)
        wsend(half, (j, 0), (2, 0), dev(dx=4 - j))
        both_z(1, j)
    cross_start(2)
    relay_z(0, 3)
    take(1, 0, 1)
    forward_start(0)
    take(0, 0, 2)
    bcast_start(1)
    relay_x(0, 3, 3)
    relay_x(0, 1, 1)
    both_x(0, 2)
    cross_start(3)
    take(0, 3, 1)
    take(0, 1, 3)
    for half in HALVES.values():
        take(half, 2, 0)
    both_z(1, 2)
    relay_z(1, 1)
    relay_z(3, 3)
    forward_start(1)
    bcast_start(2)
    relay_z(2, 1)
    for slot in ((3, 1), (1, 3), (2, 3)):
        take(1, *slot)
    take(0, 2, 3)
    take(0, 2, 1)
    own_a.wait()
    partner_a.wait_recv()

    def partner_w(zr):
        await_bytes(wbuf.at[:, 1 - c, zr], d_r.at[zr])

    partner_w(1)
    partner_w(3)

    def tile(k, zr, out):
        for j in range(4):
            for cc in CORES:
                lhs = abuf[k, :, cc, j].reshape(CR, KB)
                term = jnp.dot(lhs, wbuf[j, cc, zr], preferred_element_type=F32).astype(BF16).astype(F32)
                if j == 0 and cc == 0:
                    out[...] = term
                else:
                    out[...] += term

    def qsend(g, n):
        view = sq.at[g, t2]
        return rdma(view, view, q_s.at[g // LAST], q_r.at[g], dev(dy=n % 4, dz=n // 4))

    def square_group(g):
        for i in CORES:
            k = 2 * g + i
            if k < NK:
                await_bytes(yin.at[pl.ds(0, 3)], y_r.at[k])
            for q in range(4):
                hid = yin[q * NC + k] + rbuf[q, pl.ds(k * CR, CR), :].astype(F32)
                yin[q * NC + k] = hid
                total = jnp.sum(hid * hid, axis=1, keepdims=True)
                sq[g, t2, pl.ds(i * 4 + q, 1), :] = jnp.broadcast_to(total, (CR, 128)).T[0:1, :]
        for n in range(1, 16 if g == LAST else 4):
            qsend(g, n).start()

    def zsend(g, dz):
        view = sz.at[g, z]
        return rdma(view, view, q_s.at[0], z_r.at[g], dev(dz=dz))

    def sum_y(g):
        await_bytes(sq.at[g, pl.ds(0, 3)], q_r.at[g])
        sz[g, z] = jnp.sum(sq[g, pl.ds(z * 4, 4)], axis=0)
        for dz in AROUND:
            zsend(g, dz).start()

    def norm_group(g):
        partial = sq if g == LAST else sz
        await_bytes(partial.at[g, pl.ds(0, 15 if g == LAST else 3)], (q_r if g == LAST else z_r).at[g])
        inv_ref[g] = lax.rsqrt(jnp.sum(partial[g], axis=0) * (1.0 / 4096) + EPS_NORM)

    def step(k, carry):
        await_bytes(abuf.at[k, pl.ds(0, 2), :, pl.ds(1, 3)], f_r.at[k])
        for zr in (1, 3):
            tile(k, zr, yout.at[k, zr - 1])
            ysend(k, zr).start()

        @pl.when(k == 0)
        def _():
            relay_x(0, 3, 2)
            for n in range(4, NK):
                cross_start(n)
            both_x(0, 0)
            forward_start(2)

        @pl.when(k == 1)
        def _():
            bcast_start(3)

        @pl.when(k == 2)
        def _():
            take(0, 1, 2)
            for j in range(4):
                take(1, j, 2)
            take(0, 2, 2)
            partner_w(2)
            bcast_start(4)

        def far(i, carry):
            tile(i, 2, yout.at[i, 1])
            ysend(i, 2).start()
            return carry

        lax.fori_loop(jnp.where(k == 2, 0, k), jnp.where(k < 2, 0, k + 1), far, 0)

        @pl.when(k == 2)
        def _():
            ex_copy(0, 1 - c).start()
            for d in AROUND:
                ex_copy(d, 0).start()
            forward_start(3)
            bcast_start(5)
            forward_start(4)

        @pl.when(k == 3)
        def _():
            relay_x(0, 3, 0)
            take(0, 1, 0)
            for d in AROUND:
                ex_copy(d, 1).start()
            bcast_start(6)
            forward_start(5)

        @pl.when(k == 4)
        def _():
            forward_start(6)

        return carry

    own_r.wait()
    lax.fori_loop(0, NK, step, 0)
    take(0, 2, 0)
    partner_w(0)

    def near(i, carry):
        tile(i, 0, yin.at[z * NC + i])
        return carry

    lax.fori_loop(0, NK, near, 0)

    def ex_sum(q, carry):
        total = eout[tp, q].astype(F32)
        for d in range(1, 8):
            total += ein[(tp + d) % 8, q].astype(F32)
        yin[q * NC + NK] = total
        return carry

    for g in range(LAST):
        square_group(g)
    await_bytes(ein.at[pl.ds(0, 7)], e_r)
    lax.fori_loop(0, 4, ex_sum, 0)
    for g in range(LAST):
        sum_y(g)
    square_group(LAST)
    for g in range(LAST + 1):
        norm_group(g)

    partner_a.wait_send()
    await_bytes(abuf.at[:, :, :, pl.ds(1, 3)], a_s)
    await_bytes(yout, y_s)
    await_bytes(yin.at[pl.ds(0, 30)], w_s)
    await_bytes(yin, d_s)
    await_bytes(eout.at[pl.ds(0, 7)], e_s)
    await_bytes(sq.at[pl.ds(0, LAST), pl.ds(0, 6)], q_s.at[0])
    await_bytes(sq.at[0, pl.ds(0, 15)], q_s.at[1])


def norm_kernel(yin, inv_ref, g_ref, h_hbm, n_hbm, hbuf, nbuf, sem):
    def out_copy(k, which):
        rows = pl.ds(k * CR, CR)
        buf, dst = ((hbuf, h_hbm), (nbuf, n_hbm))[which]
        return pltpu.make_async_copy(buf.at[:, rows], dst.at[:, rows], sem.at[which])

    def chunk(k, carry):
        rows = pl.ds(k * CR, CR)
        for q in range(4):
            inv = inv_ref[k // 2, pl.ds((k % 2) * 4 + q, 1), :]
            scale = jnp.broadcast_to(inv, (128, CR)).T
            hid = yin[q * NC + k]
            hbuf[q, rows, :] = hid.astype(BF16)
            for half in CORES:
                cols = slice(half * 128, half * 128 + 128)
                nbuf[q, rows, cols] = (hid[:, cols] * scale * g_ref[:, cols]).astype(BF16)
        out_copy(k, 0).start()
        out_copy(k, 1).start()
        return carry

    lax.fori_loop(0, NC, chunk, 0)

    for which, buf in enumerate((hbuf, nbuf)):
        pltpu.make_async_copy(buf, buf, sem.at[which]).wait()


def solution(mesh):
    def local_step(attn_blk, w_blk, res_blk, gain_blk):
        any_spec = pl.BlockSpec(memory_space=pl.ANY)
        out = jax.ShapeDtypeStruct((4, NC * CR, CB), BF16)
        vmem_spec = pl.BlockSpec(memory_space=pltpu.VMEM)
        dma = pltpu.SemaphoreType.DMA
        hidden, inv = pl.pallas_call(
            kernel,
            out_shape=(pltpu.VMEM((4 * NC, CR, CB), F32), pltpu.VMEM((NC // 2, 8, 128), F32)),
            in_specs=[any_spec, any_spec, any_spec],
            out_specs=(vmem_spec, vmem_spec),
            scratch_shapes=[
                pltpu.VMEM((NK, 4, 2, 4, SUB, KB), BF16),
                pltpu.VMEM((4, 2, 4, KB, CB), BF16),
                pltpu.VMEM((NK, 3, CR, CB), F32),
                pltpu.VMEM((4, NC * CR, CB), BF16),
                pltpu.VMEM((NC // 2, 16, 8, 128), F32),
                pltpu.VMEM((NC // 2, 4, 8, 128), F32),
                pltpu.VMEM((32, 4, SUB, KB), BF16),
                pltpu.VMEM((8, 4, CR, CB), BF16),
                pltpu.VMEM((8, 4, CR, CB), BF16),
                dma((4,)),
                dma, dma((NK,)), dma, dma, dma((NK, 2)), dma((NK,)),
                dma, dma((2, 16)), dma, dma((4,)), dma, dma((NK,)),
                dma((2,)), dma((LAST + 1,)), dma, dma, dma((LAST,)),
            ],
            compiler_params=pltpu.CompilerParams(
                collective_id=0, has_side_effects=True, vmem_limit_bytes=50 * 1024 * 1024),
        )(attn_blk.reshape(8 * 4, NC, 4, SUB, KB), w_blk, res_blk.reshape(4, NC * CR, CB))
        h, n = pl.pallas_call(
            norm_kernel,
            out_shape=(out, out),
            in_specs=[vmem_spec] * 3,
            out_specs=(any_spec, any_spec),
            scratch_shapes=[pltpu.VMEM((4, NC * CR, CB), BF16)] * 2 + [dma((2,))],
            compiler_params=pltpu.CompilerParams(vmem_limit_bytes=12 * 1024 * 1024),
        )(hidden, inv, gain_blk.reshape(1, CB))
        return h.reshape(4 * NC * CR, CB), n.reshape(4 * NC * CR, CB)

    row_spec = P(("dp", "tp"), "tp2")
    return jax.shard_map(local_step, mesh=mesh, in_specs=(P("dp", "tp"), P("tp", "tp2"), row_spec, P("tp2")),
                         out_specs=(row_spec, row_spec), check_vma=False)
```

```python
import jax
import jax.numpy as jnp
from jax import lax
from jax.experimental import pallas as pl
from jax.experimental.pallas import tpu as pltpu
from jax.sharding import PartitionSpec as P

EPS_NORM = 1e-6
MESH = pl.DeviceIdType.MESH
AROUND = (1, 3, 2)
CORES = (0, 1)
BF16, F32 = jnp.bfloat16, jnp.float32

NC = 8
NK = 7
CR = 128
LAST = NC // 2 - 1
SUB = 32
KB = 512
CB = 256
PARTS = ((0, 256), (256, 256), (0, 128), (128, 128), (256, 128), (384, 128))
SIDES = ((3, 0), (1, 1))


def kernel(a_hbm, w_hbm, r_hbm, yin, hbuf, inv_ref,
           abuf, wbuf, yout, rbuf, sq, sz, ea, eout, ein,
           l_sem, a_s, a_r, p_s, p_r, b_r, f_r, w_s, w_r, d_s, d_r, y_s, y_r, q_s, q_r, e_s, e_r, z_r, h_r):
    tp, t2 = lax.axis_index("tp"), lax.axis_index("tp2")
    x, c, z, y = tp // 2, tp % 2, t2 // 4, t2 % 4

    def dev(dx=0, dy=0, dz=0, core=None):
        return {"tp": ((x + dx) % 4) * 2 + (c if core is None else core), "tp2": ((z + dz) % 4) * 4 + (y + dy) % 4}

    def rdma(src, dst, ssem, rsem, device):
        return pltpu.make_async_remote_copy(src_ref=src, dst_ref=dst, send_sem=ssem, recv_sem=rsem,
                                            device_id=device, device_id_type=MESH)

    def await_bytes(view, sem):
        pltpu.make_async_copy(view, view, sem).wait()

    ym, yp = (y + 3) % 4, (y + 1) % 4

    def cross(k, d, cd):
        return rdma(a_hbm.at[(((x + d) % 4) * 2 + cd) * 4 + z, k, y], abuf.at[k, y, c, (4 - d) % 4], a_s, a_r.at[k],
                    dev(dx=d, core=cd))

    def bcast(k, cc, back):
        view = abuf.at[k, y, cc, pl.ds(1, 3)]
        return rdma(view, view, a_s, b_r.at[k, back] if cc == back else f_r.at[k], dev(dy=3 if back else 1))

    def forward(k, back):
        view = abuf.at[k, yp if back else ym, back, pl.ds(1, 3)]
        return rdma(view, view, a_s, f_r.at[k], dev(dy=3 if back else 1))

    def ysend(k, zr):
        return rdma(yout.at[k, zr - 1], yin.at[z * NC + k], y_s, y_r.at[k], dev(dz=zr))

    def wview(part, j, zr):
        return wbuf.at[j, c, zr, pl.ds(*PARTS[part])]

    def w_arrival(part, slot):
        return w_r.at[part, slot[0] * 4 + slot[1]] if part < 2 else h_r.at[part - 2, slot[1]]

    def wsend(part, src_slot, dst_slot, device):
        rdma(wview(part, *src_slot), wview(part, *dst_slot), w_s, w_arrival(part, dst_slot), device).start()

    def dcopy(part, slot):
        view = wview(part, *slot)
        return rdma(view, view, d_s, d_r.at[slot[1]], dev(core=1 - c))

    own_a = pltpu.make_async_copy(a_hbm.at[tp * 4 + z, pl.ds(0, NK)], abuf.at[:, :, c, 0], l_sem.at[0])
    ex_a = pltpu.make_async_copy(a_hbm.at[:, NK], ea, l_sem.at[3])
    own_w = pltpu.make_async_copy(w_hbm, wbuf.at[0, c, 0], l_sem.at[1])
    own_r = pltpu.make_async_copy(r_hbm, rbuf, l_sem.at[2])
    own_w.start()
    ex_a.start()
    own_a.start()
    own_r.start()

    barrier = pltpu.get_barrier_semaphore()
    peers = [dev(dx=d, core=cd) for d in AROUND for cd in CORES] + [dev(core=1 - c)]
    peers += [dev(dy=1), dev(dy=3), dev(dz=1), dev(dz=2), dev(dz=3)]
    for peer in peers:
        pl.semaphore_signal(barrier, inc=1, device_id=peer, device_id_type=MESH)
    pl.semaphore_wait(barrier, len(peers))

    def cross_start(k):
        for d in AROUND:
            for cd in CORES:
                cross(k, d, cd).start()

    def bcast_start(k):
        await_bytes(abuf.at[k, y, :, pl.ds(1, 3)], a_r.at[k])
        for i in CORES:
            bcast(k, i, 0).start()
            bcast(k, 1 - i, 1).start()

    def forward_start(k):
        for back in CORES:
            bcast(k, back, back).wait_recv()
            forward(k, back).start()

    def take(part, j, zr):
        await_bytes(wview(part, j, zr), w_arrival(part, (j, zr)))
        dcopy(part, (j, zr)).start()

    def relay_x(part, j, zr):
        take(part, j, zr)
        wsend(part, (j, zr), (2, zr), dev(dx=4 - j))

    def pass_half(part, j, zr):
        wsend(2 + 2 * part + dict(SIDES)[j], (j, zr), (2, zr), dev(dx=4 - j))

    def take_halves(part, zr):
        for half in CORES:
            take(2 + 2 * part + half, 2, zr)

    def relay_z(j, zr):
        take(1, j, zr)
        wsend(1, (j, zr), (j, 2), dev(dz=4 - zr))

    def both_x(part, zr):
        wsend(part, (0, zr), (3, zr), dev(dx=1))
        wsend(part, (0, zr), (1, zr), dev(dx=3))

    def both_z(part, j):
        wsend(part, (j, 0), (j, 3), dev(dz=1))
        wsend(part, (j, 0), (j, 1), dev(dz=3))

    partner_a = rdma(a_hbm.at[(tp + 1 - 2 * c) * 4 + z, pl.ds(0, NK)], abuf.at[:, :, c, 0],
                     p_s, p_r, dev(core=1 - c))
    own_w.wait()
    wsend(0, (0, 0), (0, 3), dev(dz=1))
    wsend(0, (0, 0), (0, 1), dev(dz=3))
    cross_start(0)
    both_z(1, 0)
    both_x(1, 0)
    wsend(0, (0, 0), (0, 2), dev(dz=2))
    cross_start(1)
    partner_a.start()
    dcopy(0, (0, 0)).start()
    dcopy(1, (0, 0)).start()

    ex_a.wait()

    def ex_copy(d, cd):
        owner = ((x + d) % 4) * 2 + cd
        return rdma(eout.at[owner], ein.at[tp], e_s, e_r, dev(dx=d, core=cd))

    def ex_product(i, carry):
        lhs = ea[pl.ds(i * 4, 4)].reshape(4 * CR, KB)
        prod = jnp.dot(lhs, wbuf[0, c, 0], preferred_element_type=F32)
        eout[i] = prod.astype(BF16).reshape(4, CR, CB)
        return carry

    lax.fori_loop(0, 8, ex_product, 0)

    take(0, 0, 3)
    take(0, 0, 1)
    wsend(0, (0, 3), (3, 3), dev(dx=1))
    wsend(0, (0, 1), (1, 1), dev(dx=3))
    wsend(0, (0, 1), (3, 1), dev(dx=1))
    wsend(0, (0, 3), (1, 3), dev(dx=3))
    bcast_start(0)
    for j, half in SIDES:
        take(1, j, 0)
        pass_half(1, j, 0)
        both_z(1, j)
    cross_start(2)
    relay_z(0, 3)
    take(1, 0, 1)
    forward_start(0)
    take(0, 0, 2)
    bcast_start(1)
    relay_x(0, 3, 3)
    relay_x(0, 1, 1)
    both_x(0, 2)
    cross_start(3)
    take(0, 3, 1)
    take(0, 1, 3)
    take_halves(1, 0)
    both_z(1, 2)
    relay_z(1, 1)
    relay_z(3, 3)
    forward_start(1)
    bcast_start(2)
    relay_z(2, 1)
    for slot in ((3, 1), (1, 3), (2, 3)):
        take(1, *slot)
    take(0, 2, 3)
    take(0, 2, 1)
    own_a.wait()
    partner_a.wait_recv()

    def partner_w(zr):
        await_bytes(wbuf.at[:, 1 - c, zr], d_r.at[zr])

    partner_w(1)
    partner_w(3)

    def tile(k, zr, out):
        for j in range(4):
            for cc in CORES:
                lhs = abuf[k, :, cc, j].reshape(CR, KB)
                term = jnp.dot(lhs, wbuf[j, cc, zr], preferred_element_type=F32).astype(BF16).astype(F32)
                if j == 0 and cc == 0:
                    out[...] = term
                else:
                    out[...] += term

    def qsend(g, n):
        view = sq.at[g, t2]
        return rdma(view, view, q_s.at[g // LAST], q_r.at[g], dev(dy=n % 4, dz=n // 4))

    def square_group(g):
        for i in CORES:
            k = 2 * g + i
            if k < NK:
                await_bytes(yin.at[pl.ds(0, 3)], y_r.at[k])
            for q in range(4):
                hid = yin[q * NC + k] + rbuf[q, pl.ds(k * CR, CR), :].astype(F32)
                yin[q * NC + k] = hid
                hbuf[q, pl.ds(k * CR, CR), :] = hid.astype(BF16)
                total = jnp.sum(hid * hid, axis=1, keepdims=True)
                sq[g, t2, pl.ds(i * 4 + q, 1), :] = jnp.broadcast_to(total, (CR, 128)).T[0:1, :]
        for n in range(1, 16 if g == LAST else 4):
            qsend(g, n).start()

    def zsend(g, dz):
        view = sz.at[g, z]
        return rdma(view, view, q_s.at[0], z_r.at[g], dev(dz=dz))

    def sum_y(g):
        await_bytes(sq.at[g, pl.ds(0, 3)], q_r.at[g])
        sz[g, z] = jnp.sum(sq[g, pl.ds(z * 4, 4)], axis=0)
        for dz in AROUND:
            zsend(g, dz).start()

    def norm_group(g):
        partial = sq if g == LAST else sz
        await_bytes(partial.at[g, pl.ds(0, 15 if g == LAST else 3)], (q_r if g == LAST else z_r).at[g])
        inv_ref[g] = lax.rsqrt(jnp.sum(partial[g], axis=0) * (1.0 / 4096) + EPS_NORM)

    def step(k, carry):
        await_bytes(abuf.at[k, pl.ds(0, 2), :, pl.ds(1, 3)], f_r.at[k])
        for zr in (1, 3):
            tile(k, zr, yout.at[k, zr - 1])
            ysend(k, zr).start()

        @pl.when(k == 0)
        def _():
            for j, half in SIDES:
                take(0, j, 2)
                pass_half(0, j, 2)
            for n in range(4, NK):
                cross_start(n)
            both_x(0, 0)
            forward_start(2)

        @pl.when(k == 1)
        def _():
            bcast_start(3)
            for j in range(4):
                take(1, j, 2)
            take_halves(0, 2)

        @pl.when(k == 2)
        def _():
            partner_w(2)

        def far(i, carry):
            tile(i, 2, yout.at[i, 1])
            ysend(i, 2).start()
            return carry

        lax.fori_loop(jnp.where(k == 2, 0, k), jnp.where(k < 2, 0, k + 1), far, 0)

        @pl.when((k >= 2) & (k < NK - 1))
        def _():
            forward_start(k + 1)

        @pl.when((k >= 2) & (k < NK - 2))
        def _():
            bcast_start(k + 2)

        @pl.when(k == 2)
        def _():
            ex_copy(0, 1 - c).start()
            for d in AROUND:
                ex_copy(d, 0).start()

        @pl.when(k == 3)
        def _():
            for j, half in SIDES:
                take(0, j, 0)
                pass_half(0, j, 0)
            for d in AROUND:
                ex_copy(d, 1).start()

        @pl.when(k == 5)
        def _():
            take_halves(0, 0)

        return carry

    own_r.wait()
    lax.fori_loop(0, NK, step, 0)
    partner_w(0)

    def near(i, carry):
        tile(i, 0, yin.at[z * NC + i])
        return carry

    lax.fori_loop(0, NK, near, 0)

    def ex_sum(q, carry):
        total = eout[tp, q].astype(F32)
        for d in range(1, 8):
            total += ein[(tp + d) % 8, q].astype(F32)
        yin[q * NC + NK] = total
        return carry

    for g in range(LAST):
        square_group(g)
    sum_y(0)
    sum_y(1)
    await_bytes(ein.at[pl.ds(0, 7)], e_r)
    lax.fori_loop(0, 4, ex_sum, 0)
    sum_y(2)
    square_group(LAST)
    for g in range(LAST + 1):
        norm_group(g)

    partner_a.wait_send()
    await_bytes(abuf.at[:, :, :, pl.ds(1, 3)], a_s)
    await_bytes(yout, y_s)
    await_bytes(yin.at[pl.ds(0, 30)], w_s)
    await_bytes(yin, d_s)
    await_bytes(eout.at[pl.ds(0, 7)], e_s)
    await_bytes(sq.at[pl.ds(0, LAST), pl.ds(0, 6)], q_s.at[0])
    await_bytes(sq.at[0, pl.ds(0, 15)], q_s.at[1])


def norm_kernel(yin, hbuf, inv_ref, g_ref, h_hbm, n_hbm, nbuf, sem):
    h_copy = pltpu.make_async_copy(hbuf, h_hbm, sem.at[0])
    h_copy.start()

    def chunk(k, carry):
        rows = pl.ds(k * CR, CR)
        for q in range(4):
            inv = inv_ref[k // 2, pl.ds((k % 2) * 4 + q, 1), :]
            scale = jnp.broadcast_to(inv, (128, CR)).T
            for half in CORES:
                cols = pl.ds(half * 128, 128)
                nbuf[q, rows, cols] = (yin[q * NC + k, :, cols] * scale * g_ref[:, cols]).astype(BF16)
        pltpu.make_async_copy(nbuf.at[:, rows], n_hbm.at[:, rows], sem.at[1]).start()
        return carry

    lax.fori_loop(0, NC, chunk, 0)
    h_copy.wait()
    pltpu.make_async_copy(nbuf, n_hbm, sem.at[1]).wait()


def solution(mesh):
    def local_step(attn_blk, w_blk, res_blk, gain_blk):
        any_spec = pl.BlockSpec(memory_space=pl.ANY)
        out = jax.ShapeDtypeStruct((4, NC * CR, CB), BF16)
        vmem_spec = pl.BlockSpec(memory_space=pltpu.VMEM)
        dma = pltpu.SemaphoreType.DMA
        hidden, h_bf16, inv = pl.pallas_call(
            kernel,
            out_shape=(pltpu.VMEM((4 * NC, CR, CB), F32), pltpu.VMEM((4, NC * CR, CB), BF16),
                       pltpu.VMEM((NC // 2, 8, 128), F32)),
            in_specs=[any_spec, any_spec, any_spec],
            out_specs=(vmem_spec,) * 3,
            scratch_shapes=[
                pltpu.VMEM((NK, 4, 2, 4, SUB, KB), BF16),
                pltpu.VMEM((4, 2, 4, KB, CB), BF16),
                pltpu.VMEM((NK, 3, CR, CB), F32),
                pltpu.VMEM((4, NC * CR, CB), BF16),
                pltpu.VMEM((NC // 2, 16, 8, 128), F32),
                pltpu.VMEM((NC // 2, 4, 8, 128), F32),
                pltpu.VMEM((32, 4, SUB, KB), BF16),
                pltpu.VMEM((8, 4, CR, CB), BF16),
                pltpu.VMEM((8, 4, CR, CB), BF16),
                dma((4,)),
                dma, dma((NK,)), dma, dma, dma((NK, 2)), dma((NK,)),
                dma, dma((2, 16)), dma, dma((4,)), dma, dma((NK,)),
                dma((2,)), dma((LAST + 1,)), dma, dma, dma((LAST,)), dma((4, 4)),
            ],
            compiler_params=pltpu.CompilerParams(
                collective_id=0, has_side_effects=True, vmem_limit_bytes=50 * 1024 * 1024),
        )(attn_blk.reshape(8 * 4, NC, 4, SUB, KB), w_blk, res_blk.reshape(4, NC * CR, CB))
        h, n = pl.pallas_call(
            norm_kernel,
            out_shape=(out, out),
            in_specs=[vmem_spec] * 4,
            out_specs=(any_spec, any_spec),
            scratch_shapes=[pltpu.VMEM((4, NC * CR, CB), BF16), dma((2,))],
            compiler_params=pltpu.CompilerParams(vmem_limit_bytes=12 * 1024 * 1024),
        )(hidden, h_bf16, inv, gain_blk.reshape(1, CB))
        return h.reshape(4 * NC * CR, CB), n.reshape(4 * NC * CR, CB)

    row_spec = P(("dp", "tp"), "tp2")
    return jax.shard_map(local_step, mesh=mesh, in_specs=(P("dp", "tp"), P("tp", "tp2"), row_spec, P("tp2")),
                         out_specs=(row_spec, row_spec), check_vma=False)
```

```python
import jax
import jax.numpy as jnp
from jax import lax
from jax.experimental import pallas as pl
from jax.experimental.pallas import tpu as pltpu
from jax.sharding import PartitionSpec as P

EPS_NORM = 1e-6
MESH = pl.DeviceIdType.MESH
AROUND = (1, 3, 2)
CORES = (0, 1)
BF16, F32 = jnp.bfloat16, jnp.float32

NC = 8
NK = 7
CR = 128
LAST = NC // 2 - 1
SUB = 32
KB = 512
CB = 256
PARTS = ((0, 256), (256, 256), (0, 128), (128, 128), (256, 128), (384, 128))
SIDES = ((3, 0), (1, 1))


def kernel(a_hbm, w_hbm, r_hbm, yin, hbuf, inv_ref,
           abuf, wbuf, yout, rbuf, sq, sz, ea, eout, ein,
           l_sem, a_s, a_r, p_s, p_r, b_r, f_r, w_s, w_r, d_s, d_r, y_s, y_r, q_s, q_r, e_s, e_r, z_r, h_r):
    tp, t2 = lax.axis_index("tp"), lax.axis_index("tp2")
    x, c, z, y = tp // 2, tp % 2, t2 // 4, t2 % 4

    def dev(dx=0, dy=0, dz=0, core=None):
        return {"tp": ((x + dx) % 4) * 2 + (c if core is None else core), "tp2": ((z + dz) % 4) * 4 + (y + dy) % 4}

    def rdma(src, dst, ssem, rsem, device):
        return pltpu.make_async_remote_copy(src_ref=src, dst_ref=dst, send_sem=ssem, recv_sem=rsem,
                                            device_id=device, device_id_type=MESH)

    def await_bytes(view, sem):
        pltpu.make_async_copy(view, view, sem).wait()

    ym, yp = (y + 3) % 4, (y + 1) % 4

    def cross(k, d, cd):
        return rdma(a_hbm.at[(((x + d) % 4) * 2 + cd) * 4 + z, k, y], abuf.at[k, y, c, (4 - d) % 4], a_s, a_r.at[k],
                    dev(dx=d, core=cd))

    def bcast(k, cc, back):
        view = abuf.at[k, y, cc, pl.ds(1, 3)]
        return rdma(view, view, a_s, b_r.at[k, back] if cc == back else f_r.at[k], dev(dy=3 if back else 1))

    def forward(k, back):
        view = abuf.at[k, yp if back else ym, back, pl.ds(1, 3)]
        return rdma(view, view, a_s, f_r.at[k], dev(dy=3 if back else 1))

    def ysend(k, zr):
        return rdma(yout.at[k, zr - 1], yin.at[z * NC + k], y_s, y_r.at[k], dev(dz=zr))

    def wview(part, j, zr):
        return wbuf.at[j, c, zr, pl.ds(*PARTS[part])]

    def w_arrival(part, slot):
        return w_r.at[part, slot[0] * 4 + slot[1]] if part < 2 else h_r.at[part - 2, slot[1] // 2]

    def wsend(part, src_slot, dst_slot, device):
        rdma(wview(part, *src_slot), wview(part, *dst_slot), w_s, w_arrival(part, dst_slot), device).start()

    def dcopy(part, slot):
        view = wview(part, *slot)
        return rdma(view, view, d_s, d_r.at[slot[1]], dev(core=1 - c))

    own_a = pltpu.make_async_copy(a_hbm.at[tp * 4 + z, pl.ds(0, NK)], abuf.at[:, :, c, 0], l_sem.at[0])
    ex_a = pltpu.make_async_copy(a_hbm.at[:, NK], ea, l_sem.at[3])
    own_w = pltpu.make_async_copy(w_hbm, wbuf.at[0, c, 0], l_sem.at[1])
    own_r = pltpu.make_async_copy(r_hbm, rbuf, l_sem.at[2])
    own_w.start()
    ex_a.start()
    own_a.start()
    own_r.start()

    barrier = pltpu.get_barrier_semaphore()
    peers = [dev(dx=d, core=cd) for d in AROUND for cd in CORES] + [dev(core=1 - c)]
    peers += [dev(dy=1), dev(dy=3), dev(dz=1), dev(dz=2), dev(dz=3)]
    for peer in peers:
        pl.semaphore_signal(barrier, inc=1, device_id=peer, device_id_type=MESH)
    pl.semaphore_wait(barrier, len(peers))

    def cross_start(k):
        for d in AROUND:
            for cd in CORES:
                cross(k, d, cd).start()

    def bcast_start(k):
        await_bytes(abuf.at[k, y, :, pl.ds(1, 3)], a_r.at[k])
        for i in CORES:
            bcast(k, i, 0).start()
            bcast(k, 1 - i, 1).start()

    def forward_start(k):
        for back in CORES:
            bcast(k, back, back).wait_recv()
            forward(k, back).start()

    def take(part, j, zr):
        await_bytes(wview(part, j, zr), w_arrival(part, (j, zr)))
        dcopy(part, (j, zr)).start()

    def relay_x(part, j, zr):
        take(part, j, zr)
        wsend(part, (j, zr), (2, zr), dev(dx=4 - j))

    def pass_half(part, j, zr):
        wsend(2 + 2 * part + dict(SIDES)[j], (j, zr), (2, zr), dev(dx=4 - j))

    def take_halves(part, zr):
        for half in CORES:
            take(2 + 2 * part + half, 2, zr)

    def relay_z(j, zr):
        take(1, j, zr)
        wsend(1, (j, zr), (j, 2), dev(dz=4 - zr))

    def both_x(part, zr):
        wsend(part, (0, zr), (3, zr), dev(dx=1))
        wsend(part, (0, zr), (1, zr), dev(dx=3))

    def both_z(part, j):
        wsend(part, (j, 0), (j, 3), dev(dz=1))
        wsend(part, (j, 0), (j, 1), dev(dz=3))

    partner_a = rdma(a_hbm.at[(tp + 1 - 2 * c) * 4 + z, pl.ds(0, NK)], abuf.at[:, :, c, 0],
                     p_s, p_r, dev(core=1 - c))
    own_w.wait()
    wsend(0, (0, 0), (0, 3), dev(dz=1))
    wsend(0, (0, 0), (0, 1), dev(dz=3))
    both_x(1, 0)
    cross_start(0)
    both_z(1, 0)
    wsend(0, (0, 0), (0, 2), dev(dz=2))
    cross_start(1)
    partner_a.start()
    dcopy(0, (0, 0)).start()
    dcopy(1, (0, 0)).start()

    ex_a.wait()

    def ex_copy(d, cd):
        owner = ((x + d) % 4) * 2 + cd
        return rdma(eout.at[owner], ein.at[tp], e_s, e_r, dev(dx=d, core=cd))

    def ex_product(i, carry):
        lhs = ea[pl.ds(i * 4, 4)].reshape(4 * CR, KB)
        prod = jnp.dot(lhs, wbuf[0, c, 0], preferred_element_type=F32)
        eout[i] = prod.astype(BF16).reshape(4, CR, CB)
        return carry

    lax.fori_loop(0, 8, ex_product, 0)

    take(0, 0, 3)
    take(0, 0, 1)
    wsend(0, (0, 3), (3, 3), dev(dx=1))
    wsend(0, (0, 1), (1, 1), dev(dx=3))
    wsend(0, (0, 1), (3, 1), dev(dx=1))
    wsend(0, (0, 3), (1, 3), dev(dx=3))
    bcast_start(0)
    for j, half in SIDES:
        take(1, j, 0)
        pass_half(1, j, 0)
        both_z(1, j)
    cross_start(2)
    relay_z(0, 3)
    take(1, 0, 1)
    forward_start(0)
    take(0, 0, 2)
    bcast_start(1)
    relay_x(0, 3, 3)
    relay_x(0, 1, 1)
    both_x(0, 2)
    cross_start(3)
    take(0, 3, 1)
    take(0, 1, 3)
    take_halves(1, 0)
    both_z(1, 2)
    relay_z(1, 1)
    relay_z(3, 3)
    forward_start(1)
    bcast_start(2)
    relay_z(2, 1)
    for slot in ((3, 1), (1, 3), (2, 3)):
        take(1, *slot)
    take(0, 2, 3)
    take(0, 2, 1)
    own_a.wait()
    partner_a.wait_recv()

    def partner_w(zr):
        await_bytes(wbuf.at[:, 1 - c, zr], d_r.at[zr])

    partner_w(1)
    partner_w(3)

    def tile(k, zr, out):
        for j in range(4):
            for cc in CORES:
                lhs = abuf[k, :, cc, j].reshape(CR, KB)
                term = jnp.dot(lhs, wbuf[j, cc, zr], preferred_element_type=F32).astype(BF16).astype(F32)
                if j == 0 and cc == 0:
                    out[...] = term
                else:
                    out[...] += term

    def qsend(g, n):
        view = sq.at[g, t2]
        return rdma(view, view, q_s.at[g // LAST], q_r.at[g], dev(dy=n % 4, dz=n // 4))

    def square_group(g):
        for i in (1, 0) if g == LAST else CORES:
            k = 2 * g + i
            if k < NK:
                await_bytes(yin.at[pl.ds(0, 3)], y_r.at[k])
            for q in range(4):
                hid = yin[q * NC + k] + rbuf[q, pl.ds(k * CR, CR), :].astype(F32)
                yin[q * NC + k] = hid
                hbuf[q, pl.ds(k * CR, CR), :] = hid.astype(BF16)
                total = jnp.sum(hid * hid, axis=1, keepdims=True)
                sq[g, t2, pl.ds(i * 4 + q, 1), :] = jnp.broadcast_to(total, (CR, 128)).T[0:1, :]
        for n in range(1, 16 if g == LAST else 4):
            qsend(g, n).start()

    def zsend(g, dz):
        view = sz.at[g, z]
        return rdma(view, view, q_s.at[0], z_r.at[g], dev(dz=dz))

    def sum_y(g):
        await_bytes(sq.at[g, pl.ds(0, 3)], q_r.at[g])
        sz[g, z] = jnp.sum(sq[g, pl.ds(z * 4, 4)], axis=0)
        for dz in AROUND:
            zsend(g, dz).start()

    def norm_group(g):
        partial = sq if g == LAST else sz
        await_bytes(partial.at[g, pl.ds(0, 15 if g == LAST else 3)], (q_r if g == LAST else z_r).at[g])
        inv_ref[g] = lax.rsqrt(jnp.sum(partial[g], axis=0) * (1.0 / 4096) + EPS_NORM)

    def step(k, carry):
        await_bytes(abuf.at[k, pl.ds(0, 2), :, pl.ds(1, 3)], f_r.at[k])
        for zr in (1, 3):
            tile(k, zr, yout.at[k, zr - 1])
            ysend(k, zr).start()

        @pl.when(k == 0)
        def _():
            for j, half in SIDES:
                take(0, j, 2)
                pass_half(0, j, 2)
            cross_start(4)
            forward_start(2)

        @pl.when(k == 1)
        def _():
            bcast_start(3)
            for n in range(5, NK):
                cross_start(n)
            both_x(0, 0)
            for j in range(4):
                take(1, j, 2)
            take_halves(0, 2)

        @pl.when(k == 2)
        def _():
            partner_w(2)

        def far(i, carry):
            tile(i, 2, yout.at[i, 1])
            ysend(i, 2).start()
            return carry

        lax.fori_loop(jnp.where(k == 2, 0, k), jnp.where(k < 2, 0, k + 1), far, 0)

        @pl.when((k >= 2) & (k < NK - 1))
        def _():
            forward_start(k + 1)

        @pl.when((k >= 2) & (k < NK - 2))
        def _():
            bcast_start(k + 2)

        @pl.when(k == 2)
        def _():
            ex_copy(0, 1 - c).start()
            for d in AROUND:
                ex_copy(d, 0).start()

        @pl.when(k == 3)
        def _():
            for j, half in SIDES:
                take(0, j, 0)
                pass_half(0, j, 0)
            for d in AROUND:
                ex_copy(d, 1).start()

        @pl.when(k == 5)
        def _():
            take_halves(0, 0)

        return carry

    own_r.wait()
    lax.fori_loop(0, NK, step, 0)
    partner_w(0)

    def near(i, carry):
        tile(i, 0, yin.at[z * NC + i])
        return carry

    lax.fori_loop(0, NK, near, 0)

    def ex_sum(q, carry):
        total = eout[tp, q].astype(F32)
        for d in range(1, 8):
            total += ein[(tp + d) % 8, q].astype(F32)
        yin[q * NC + NK] = total
        return carry

    for g in range(LAST):
        square_group(g)
    sum_y(0)
    sum_y(1)
    await_bytes(ein.at[pl.ds(0, 7)], e_r)
    lax.fori_loop(0, 4, ex_sum, 0)
    sum_y(2)
    square_group(LAST)
    for g in range(LAST + 1):
        norm_group(g)

    partner_a.wait_send()
    await_bytes(abuf.at[:, :, :, pl.ds(1, 3)], a_s)
    await_bytes(yout, y_s)
    await_bytes(yin.at[pl.ds(0, 30)], w_s)
    await_bytes(yin, d_s)
    await_bytes(eout.at[pl.ds(0, 7)], e_s)
    await_bytes(sq.at[pl.ds(0, LAST), pl.ds(0, 6)], q_s.at[0])
    await_bytes(sq.at[0, pl.ds(0, 15)], q_s.at[1])


def norm_kernel(yin, hbuf, inv_ref, g_ref, h_hbm, n_hbm, nbuf, sem):
    h_copy = pltpu.make_async_copy(hbuf, h_hbm, sem.at[0])
    h_copy.start()

    def chunk(k, carry):
        rows = pl.ds(k * CR, CR)
        for q in range(4):
            inv = inv_ref[k // 2, pl.ds((k % 2) * 4 + q, 1), :]
            scale = jnp.broadcast_to(inv, (128, CR)).T
            for half in CORES:
                cols = pl.ds(half * 128, 128)
                nbuf[q, rows, cols] = (yin[q * NC + k, :, cols] * scale * g_ref[:, cols]).astype(BF16)
        pltpu.make_async_copy(nbuf.at[:, rows], n_hbm.at[:, rows], sem.at[1]).start()
        return carry

    lax.fori_loop(0, NC, chunk, 0)
    h_copy.wait()
    pltpu.make_async_copy(nbuf, n_hbm, sem.at[1]).wait()


def solution(mesh):
    def local_step(attn_blk, w_blk, res_blk, gain_blk):
        any_spec = pl.BlockSpec(memory_space=pl.ANY)
        out = jax.ShapeDtypeStruct((4, NC * CR, CB), BF16)
        vmem_spec = pl.BlockSpec(memory_space=pltpu.VMEM)
        dma = pltpu.SemaphoreType.DMA
        hidden, h_bf16, inv = pl.pallas_call(
            kernel,
            out_shape=(pltpu.VMEM((4 * NC, CR, CB), F32), pltpu.VMEM((4, NC * CR, CB), BF16),
                       pltpu.VMEM((NC // 2, 8, 128), F32)),
            in_specs=[any_spec, any_spec, any_spec],
            out_specs=(vmem_spec,) * 3,
            scratch_shapes=[
                pltpu.VMEM((NK, 4, 2, 4, SUB, KB), BF16),
                pltpu.VMEM((4, 2, 4, KB, CB), BF16),
                pltpu.VMEM((NK, 3, CR, CB), F32),
                pltpu.VMEM((4, NC * CR, CB), BF16),
                pltpu.VMEM((NC // 2, 16, 8, 128), F32),
                pltpu.VMEM((NC // 2, 4, 8, 128), F32),
                pltpu.VMEM((32, 4, SUB, KB), BF16),
                pltpu.VMEM((8, 4, CR, CB), BF16),
                pltpu.VMEM((8, 4, CR, CB), BF16),
                dma((4,)),
                dma, dma((NK,)), dma, dma, dma((NK, 2)), dma((NK,)),
                dma, dma((2, 16)), dma, dma((4,)), dma, dma((NK,)),
                dma((2,)), dma((LAST + 1,)), dma, dma, dma((LAST,)), dma((4, 2)),
            ],
            compiler_params=pltpu.CompilerParams(
                collective_id=0, has_side_effects=True, vmem_limit_bytes=50 * 1024 * 1024),
        )(attn_blk.reshape(8 * 4, NC, 4, SUB, KB), w_blk, res_blk.reshape(4, NC * CR, CB))
        h, n = pl.pallas_call(
            norm_kernel,
            out_shape=(out, out),
            in_specs=[vmem_spec] * 4,
            out_specs=(any_spec, any_spec),
            scratch_shapes=[pltpu.VMEM((4, NC * CR, CB), BF16), dma((2,))],
            compiler_params=pltpu.CompilerParams(vmem_limit_bytes=12 * 1024 * 1024),
        )(hidden, h_bf16, inv, gain_blk.reshape(1, CB))
        return h.reshape(4 * NC * CR, CB), n.reshape(4 * NC * CR, CB)

    row_spec = P(("dp", "tp"), "tp2")
    return jax.shard_map(local_step, mesh=mesh, in_specs=(P("dp", "tp"), P("tp", "tp2"), row_spec, P("tp2")),
                         out_specs=(row_spec, row_spec), check_vma=False)
```

```python
import jax
import jax.numpy as jnp
from jax import lax
from jax.experimental import pallas as pl
from jax.experimental.pallas import tpu as pltpu
from jax.sharding import PartitionSpec as P

EPS_NORM = 1e-6
MESH = pl.DeviceIdType.MESH
AROUND = (1, 3, 2)
CORES = (0, 1)
FAR_FIRST = sorted(range(1, 16), key=lambda n: (n % 4 != 2) + (n % 4 == 0) + (n // 4 != 2) + (n // 4 == 0))
BF16, F32 = jnp.bfloat16, jnp.float32

NC = 8
NK = 7
CR = 128
LAST = NC // 2 - 1
SUB = 32
KB = 512
CB = 256
PARTS = ((0, 256), (256, 256), (0, 128), (128, 128), (256, 128), (384, 128))
SIDES = ((3, 0), (1, 1))


def kernel(a_hbm, w_hbm, r_hbm, yin, hbuf, inv_ref,
           abuf, wbuf, yout, rbuf, sq, sz, ea, eout, ein,
           l_sem, a_s, a_r, p_s, p_r, b_r, f_r, w_s, w_r, d_s, d_r, y_s, y_r, q_s, q_r, e_s, e_r, z_r, h_r):
    tp, t2 = lax.axis_index("tp"), lax.axis_index("tp2")
    x, c, z, y = tp // 2, tp % 2, t2 // 4, t2 % 4

    def dev(dx=0, dy=0, dz=0, core=None):
        return {"tp": ((x + dx) % 4) * 2 + (c if core is None else core), "tp2": ((z + dz) % 4) * 4 + (y + dy) % 4}

    def rdma(src, dst, ssem, rsem, device):
        return pltpu.make_async_remote_copy(src_ref=src, dst_ref=dst, send_sem=ssem, recv_sem=rsem,
                                            device_id=device, device_id_type=MESH)

    def await_bytes(view, sem):
        pltpu.make_async_copy(view, view, sem).wait()

    ym, yp = (y + 3) % 4, (y + 1) % 4

    def cross(k, d, cd):
        return rdma(a_hbm.at[(((x + d) % 4) * 2 + cd) * 4 + z, k, y], abuf.at[k, y, c, (4 - d) % 4], a_s, a_r.at[k],
                    dev(dx=d, core=cd))

    def bcast(k, cc, back):
        view = abuf.at[k, y, cc, pl.ds(1, 3)]
        return rdma(view, view, a_s, b_r.at[k, back] if cc == back else f_r.at[k], dev(dy=3 if back else 1))

    def forward(k, back):
        view = abuf.at[k, yp if back else ym, back, pl.ds(1, 3)]
        return rdma(view, view, a_s, f_r.at[k], dev(dy=3 if back else 1))

    def ysend(k, zr):
        return rdma(yout.at[k, zr - 1], yin.at[z * NC + k], y_s, y_r.at[k], dev(dz=zr))

    def wview(part, j, zr):
        return wbuf.at[j, c, zr, pl.ds(*PARTS[part])]

    def w_arrival(part, slot):
        return w_r.at[part, slot[0] * 4 + slot[1]] if part < 2 else h_r.at[part - 2, slot[1] // 2]

    def wsend(part, src_slot, dst_slot, device):
        rdma(wview(part, *src_slot), wview(part, *dst_slot), w_s, w_arrival(part, dst_slot), device).start()

    def dcopy(part, slot):
        view = wview(part, *slot)
        return rdma(view, view, d_s, d_r.at[slot[1]], dev(core=1 - c))

    own_a = pltpu.make_async_copy(a_hbm.at[tp * 4 + z, pl.ds(0, NK)], abuf.at[:, :, c, 0], l_sem.at[0])
    ex_a = pltpu.make_async_copy(a_hbm.at[:, NK], ea, l_sem.at[3])
    own_w = pltpu.make_async_copy(w_hbm, wbuf.at[0, c, 0], l_sem.at[1])
    own_r = pltpu.make_async_copy(r_hbm, rbuf, l_sem.at[2])
    own_w.start()
    ex_a.start()
    own_a.start()
    own_r.start()

    barrier = pltpu.get_barrier_semaphore()
    peers = [dev(dx=d, core=cd) for d in AROUND for cd in CORES] + [dev(core=1 - c)]
    peers += [dev(dy=1), dev(dy=3), dev(dz=1), dev(dz=2), dev(dz=3)]
    for peer in peers:
        pl.semaphore_signal(barrier, inc=1, device_id=peer, device_id_type=MESH)
    pl.semaphore_wait(barrier, len(peers))

    def cross_start(k):
        for d in AROUND:
            for cd in CORES:
                cross(k, d, cd).start()

    def bcast_start(k):
        await_bytes(abuf.at[k, y, :, pl.ds(1, 3)], a_r.at[k])
        for i in CORES:
            bcast(k, i, 0).start()
            bcast(k, 1 - i, 1).start()

    def forward_start(k):
        for back in CORES:
            bcast(k, back, back).wait_recv()
            forward(k, back).start()

    def take(part, j, zr):
        await_bytes(wview(part, j, zr), w_arrival(part, (j, zr)))
        dcopy(part, (j, zr)).start()

    def relay_x(part, j, zr):
        take(part, j, zr)
        wsend(part, (j, zr), (2, zr), dev(dx=4 - j))

    def pass_half(part, j, zr):
        wsend(2 + 2 * part + dict(SIDES)[j], (j, zr), (2, zr), dev(dx=4 - j))

    def take_halves(part, zr):
        for half in CORES:
            take(2 + 2 * part + half, 2, zr)

    def relay_z(j, zr):
        take(1, j, zr)
        wsend(1, (j, zr), (j, 2), dev(dz=4 - zr))

    def both_x(part, zr):
        wsend(part, (0, zr), (3, zr), dev(dx=1))
        wsend(part, (0, zr), (1, zr), dev(dx=3))

    def both_z(part, j):
        wsend(part, (j, 0), (j, 3), dev(dz=1))
        wsend(part, (j, 0), (j, 1), dev(dz=3))

    partner_a = rdma(a_hbm.at[(tp + 1 - 2 * c) * 4 + z, pl.ds(0, NK)], abuf.at[:, :, c, 0],
                     p_s, p_r, dev(core=1 - c))
    own_w.wait()
    wsend(0, (0, 0), (0, 3), dev(dz=1))
    wsend(0, (0, 0), (0, 1), dev(dz=3))
    both_x(1, 0)
    cross_start(0)
    both_z(1, 0)
    wsend(0, (0, 0), (0, 2), dev(dz=2))
    cross_start(1)
    partner_a.start()
    dcopy(0, (0, 0)).start()
    dcopy(1, (0, 0)).start()

    ex_a.wait()

    def ex_copy(d, cd):
        owner = ((x + d) % 4) * 2 + cd
        return rdma(eout.at[owner], ein.at[tp], e_s, e_r, dev(dx=d, core=cd))

    def ex_product(i, carry):
        lhs = ea[pl.ds(i * 4, 4)].reshape(4 * CR, KB)
        prod = jnp.dot(lhs, wbuf[0, c, 0], preferred_element_type=F32)
        eout[i] = prod.astype(BF16).reshape(4, CR, CB)
        return carry

    lax.fori_loop(0, 8, ex_product, 0)

    take(0, 0, 3)
    take(0, 0, 1)
    wsend(0, (0, 3), (3, 3), dev(dx=1))
    wsend(0, (0, 1), (1, 1), dev(dx=3))
    wsend(0, (0, 1), (3, 1), dev(dx=1))
    wsend(0, (0, 3), (1, 3), dev(dx=3))
    bcast_start(0)
    for j, half in SIDES:
        take(1, j, 0)
        pass_half(1, j, 0)
        both_z(1, j)
    cross_start(2)
    relay_z(0, 3)
    take(1, 0, 1)
    forward_start(0)
    take(0, 0, 2)
    bcast_start(1)
    relay_x(0, 3, 3)
    relay_x(0, 1, 1)
    both_x(0, 2)
    cross_start(3)
    take(0, 3, 1)
    take(0, 1, 3)
    take_halves(1, 0)
    both_z(1, 2)
    relay_z(1, 1)
    relay_z(3, 3)
    forward_start(1)
    bcast_start(2)
    relay_z(2, 1)
    for slot in ((3, 1), (1, 3), (2, 3)):
        take(1, *slot)
    take(0, 2, 3)
    take(0, 2, 1)
    own_a.wait()
    partner_a.wait_recv()

    def partner_w(zr):
        await_bytes(wbuf.at[:, 1 - c, zr], d_r.at[zr])

    partner_w(1)
    partner_w(3)

    def tile(k, zr, out):
        for j in range(4):
            for cc in CORES:
                lhs = abuf[k, :, cc, j].reshape(CR, KB)
                term = jnp.dot(lhs, wbuf[j, cc, zr], preferred_element_type=F32).astype(BF16).astype(F32)
                if j == 0 and cc == 0:
                    out[...] = term
                else:
                    out[...] += term

    def qsend(g, n):
        view = sq.at[g, t2]
        return rdma(view, view, q_s.at[g // LAST], q_r.at[g], dev(dy=n % 4, dz=n // 4))

    def square_group(g):
        for i in (1, 0) if g == LAST else CORES:
            k = 2 * g + i
            if k < NK:
                await_bytes(yin.at[pl.ds(0, 3)], y_r.at[k])
            for q in range(4):
                hid = yin[q * NC + k] + rbuf[q, pl.ds(k * CR, CR), :].astype(F32)
                yin[q * NC + k] = hid
                hbuf[q, pl.ds(k * CR, CR), :] = hid.astype(BF16)
                total = jnp.sum(hid * hid, axis=1, keepdims=True)
                sq[g, t2, pl.ds(i * 4 + q, 1), :] = jnp.broadcast_to(total, (CR, 128)).T[0:1, :]
        for n in FAR_FIRST if g == LAST else AROUND:
            qsend(g, n).start()

    def zsend(g, dz):
        view = sz.at[g, z]
        return rdma(view, view, q_s.at[0], z_r.at[g], dev(dz=dz))

    def sum_y(g):
        await_bytes(sq.at[g, pl.ds(0, 3)], q_r.at[g])
        sz[g, z] = jnp.sum(sq[g, pl.ds(z * 4, 4)], axis=0)
        for dz in AROUND:
            zsend(g, dz).start()

    def norm_group(g):
        partial = sq if g == LAST else sz
        await_bytes(partial.at[g, pl.ds(0, 15 if g == LAST else 3)], (q_r if g == LAST else z_r).at[g])
        inv_ref[g] = lax.rsqrt(jnp.sum(partial[g], axis=0) * (1.0 / 4096) + EPS_NORM)

    def step(k, carry):
        await_bytes(abuf.at[k, pl.ds(0, 2), :, pl.ds(1, 3)], f_r.at[k])
        for zr in (1, 3):
            tile(k, zr, yout.at[k, zr - 1])
            ysend(k, zr).start()

        @pl.when(k == 0)
        def _():
            for j, half in SIDES:
                take(0, j, 2)
                pass_half(0, j, 2)
            cross_start(4)
            forward_start(2)

        @pl.when(k == 1)
        def _():
            bcast_start(3)
            for n in range(5, NK):
                cross_start(n)
            both_x(0, 0)
            for j in range(4):
                take(1, j, 2)
            take_halves(0, 2)

        @pl.when(k == 2)
        def _():
            partner_w(2)

        def far(i, carry):
            tile(i, 2, yout.at[i, 1])
            ysend(i, 2).start()
            return carry

        lax.fori_loop(jnp.where(k == 2, 0, k), jnp.where(k < 2, 0, k + 1), far, 0)

        @pl.when((k >= 2) & (k < NK - 1))
        def _():
            forward_start(k + 1)

        @pl.when((k >= 2) & (k < NK - 2))
        def _():
            bcast_start(k + 2)

        @pl.when(k == 2)
        def _():
            ex_copy(0, 1 - c).start()
            for d in AROUND:
                ex_copy(d, 0).start()

        @pl.when(k == 3)
        def _():
            for j, half in SIDES:
                take(0, j, 0)
                pass_half(0, j, 0)
            for d in AROUND:
                ex_copy(d, 1).start()

        @pl.when(k == 5)
        def _():
            take_halves(0, 0)

        return carry

    own_r.wait()
    lax.fori_loop(0, NK, step, 0)
    partner_w(0)

    def near(i, carry):
        tile(i, 0, yin.at[z * NC + i])
        return carry

    lax.fori_loop(0, NK, near, 0)

    def ex_sum(q, carry):
        total = eout[tp, q].astype(F32)
        for d in range(1, 8):
            total += ein[(tp + d) % 8, q].astype(F32)
        yin[q * NC + NK] = total
        return carry

    for g in range(LAST):
        square_group(g)
    sum_y(0)
    sum_y(1)
    await_bytes(ein.at[pl.ds(0, 7)], e_r)
    lax.fori_loop(0, 4, ex_sum, 0)
    sum_y(2)
    square_group(LAST)
    for g in range(LAST + 1):
        norm_group(g)

    partner_a.wait_send()
    await_bytes(abuf.at[:, :, :, pl.ds(1, 3)], a_s)
    await_bytes(yout, y_s)
    await_bytes(yin.at[pl.ds(0, 30)], w_s)
    await_bytes(yin, d_s)
    await_bytes(eout.at[pl.ds(0, 7)], e_s)
    await_bytes(sq.at[pl.ds(0, LAST), pl.ds(0, 6)], q_s.at[0])
    await_bytes(sq.at[0, pl.ds(0, 15)], q_s.at[1])


def norm_kernel(yin, hbuf, inv_ref, g_ref, h_hbm, n_hbm, nbuf, sem):
    h_copy = pltpu.make_async_copy(hbuf, h_hbm, sem.at[0])
    h_copy.start()

    def chunk(k, carry):
        rows = pl.ds(k * CR, CR)
        for q in range(4):
            inv = inv_ref[k // 2, pl.ds((k % 2) * 4 + q, 1), :]
            scale = jnp.broadcast_to(inv, (128, CR)).T
            for half in CORES:
                cols = pl.ds(half * 128, 128)
                nbuf[q, rows, cols] = (yin[q * NC + k, :, cols] * scale * g_ref[:, cols]).astype(BF16)
        pltpu.make_async_copy(nbuf.at[:, rows], n_hbm.at[:, rows], sem.at[1]).start()
        return carry

    lax.fori_loop(0, NC, chunk, 0)
    h_copy.wait()
    pltpu.make_async_copy(nbuf, n_hbm, sem.at[1]).wait()


def solution(mesh):
    def local_step(attn_blk, w_blk, res_blk, gain_blk):
        any_spec = pl.BlockSpec(memory_space=pl.ANY)
        out = jax.ShapeDtypeStruct((4, NC * CR, CB), BF16)
        vmem_spec = pl.BlockSpec(memory_space=pltpu.VMEM)
        dma = pltpu.SemaphoreType.DMA
        hidden, h_bf16, inv = pl.pallas_call(
            kernel,
            out_shape=(pltpu.VMEM((4 * NC, CR, CB), F32), pltpu.VMEM((4, NC * CR, CB), BF16),
                       pltpu.VMEM((NC // 2, 8, 128), F32)),
            in_specs=[any_spec, any_spec, any_spec],
            out_specs=(vmem_spec,) * 3,
            scratch_shapes=[
                pltpu.VMEM((NK, 4, 2, 4, SUB, KB), BF16),
                pltpu.VMEM((4, 2, 4, KB, CB), BF16),
                pltpu.VMEM((NK, 3, CR, CB), F32),
                pltpu.VMEM((4, NC * CR, CB), BF16),
                pltpu.VMEM((NC // 2, 16, 8, 128), F32),
                pltpu.VMEM((NC // 2, 4, 8, 128), F32),
                pltpu.VMEM((32, 4, SUB, KB), BF16),
                pltpu.VMEM((8, 4, CR, CB), BF16),
                pltpu.VMEM((8, 4, CR, CB), BF16),
                dma((4,)),
                dma, dma((NK,)), dma, dma, dma((NK, 2)), dma((NK,)),
                dma, dma((2, 16)), dma, dma((4,)), dma, dma((NK,)),
                dma((2,)), dma((LAST + 1,)), dma, dma, dma((LAST,)), dma((4, 2)),
            ],
            compiler_params=pltpu.CompilerParams(
                collective_id=0, has_side_effects=True, vmem_limit_bytes=50 * 1024 * 1024),
        )(attn_blk.reshape(8 * 4, NC, 4, SUB, KB), w_blk, res_blk.reshape(4, NC * CR, CB))
        h, n = pl.pallas_call(
            norm_kernel,
            out_shape=(out, out),
            in_specs=[vmem_spec] * 4,
            out_specs=(any_spec, any_spec),
            scratch_shapes=[pltpu.VMEM((4, NC * CR, CB), BF16), dma((2,))],
            compiler_params=pltpu.CompilerParams(vmem_limit_bytes=12 * 1024 * 1024),
        )(hidden, h_bf16, inv, gain_blk.reshape(1, CB))
        return h.reshape(4 * NC * CR, CB), n.reshape(4 * NC * CR, CB)

    row_spec = P(("dp", "tp"), "tp2")
    return jax.shard_map(local_step, mesh=mesh, in_specs=(P("dp", "tp"), P("tp", "tp2"), row_spec, P("tp2")),
                         out_specs=(row_spec, row_spec), check_vma=False)
```

```python
import jax
import jax.numpy as jnp
from jax import lax
from jax.experimental import pallas as pl
from jax.experimental.pallas import tpu as pltpu
from jax.sharding import PartitionSpec as P

EPS_NORM = 1e-6
MESH = pl.DeviceIdType.MESH
AROUND = (1, 3, 2)
CORES = (0, 1)
FAR_FIRST = sorted(range(1, 16), key=lambda n: (n % 4 != 2) + (n % 4 == 0) + (n // 4 != 2) + (n // 4 == 0))
BF16, F32 = jnp.bfloat16, jnp.float32

NC = 8
NK = 7
CR = 128
LAST = NC // 2 - 1
SUB = 32
KB = 512
CB = 256
PARTS = ((0, 256), (256, 256), (0, 128), (128, 128), (256, 128), (384, 128))
SIDES = ((3, 0), (1, 1))


def kernel(a_hbm, w_hbm, r_hbm, yin, hbuf, inv_ref,
           abuf, wbuf, yout, rbuf, sq, sz, ea, eout, ein,
           l_sem, a_s, a_r, p_s, p_r, b_r, f_r, w_s, w_r, d_s, d_r, y_s, y_r, q_s, q_r, e_s, e_r, z_r):
    tp, t2 = lax.axis_index("tp"), lax.axis_index("tp2")
    x, c, z, y = tp // 2, tp % 2, t2 // 4, t2 % 4

    def dev(dx=0, dy=0, dz=0, core=None):
        return {"tp": ((x + dx) % 4) * 2 + (c if core is None else core), "tp2": ((z + dz) % 4) * 4 + (y + dy) % 4}

    def rdma(src, dst, ssem, rsem, device):
        return pltpu.make_async_remote_copy(src_ref=src, dst_ref=dst, send_sem=ssem, recv_sem=rsem,
                                            device_id=device, device_id_type=MESH)

    def await_bytes(view, sem):
        pltpu.make_async_copy(view, view, sem).wait()

    ym, yp = (y + 3) % 4, (y + 1) % 4

    def cross(k, d, cd):
        return rdma(a_hbm.at[(((x + d) % 4) * 2 + cd) * 4 + z, k, y], abuf.at[k, y, c, (4 - d) % 4], a_s, a_r.at[k],
                    dev(dx=d, core=cd))

    def bcast(k, cc, back):
        view = abuf.at[k, y, cc, pl.ds(1, 3)]
        return rdma(view, view, a_s, b_r.at[k, back] if cc == back else f_r.at[k], dev(dy=3 if back else 1))

    def forward(k, back):
        view = abuf.at[k, yp if back else ym, back, pl.ds(1, 3)]
        return rdma(view, view, a_s, f_r.at[k], dev(dy=3 if back else 1))

    def ysend(k, zr):
        return rdma(yout.at[k, zr - 1], yin.at[z * NC + k], y_s, y_r.at[k], dev(dz=zr))

    def wview(part, j, zr):
        return wbuf.at[j, c, zr, pl.ds(*PARTS[part])]

    w_index = {}

    def w_arrival(part, slot):
        if part > 1:
            key = (part // 2, slot[1])
        else:
            key = (part, "far") if part == 1 and slot[1] == 2 else (part, slot)
        return w_r.at[w_index.setdefault(key, len(w_index))]

    def wsend(part, src_slot, dst_slot, device):
        rdma(wview(part, *src_slot), wview(part, *dst_slot), w_s, w_arrival(part, dst_slot), device).start()

    def dcopy(part, slot):
        view = wview(part, *slot)
        return rdma(view, view, d_s, d_r.at[slot[1]], dev(core=1 - c))

    own_a = pltpu.make_async_copy(a_hbm.at[tp * 4 + z, pl.ds(0, NK)], abuf.at[:, :, c, 0], l_sem.at[0])
    ex_a = pltpu.make_async_copy(a_hbm.at[:, NK], ea, l_sem.at[3])
    own_w = pltpu.make_async_copy(w_hbm, wbuf.at[0, c, 0], l_sem.at[1])
    own_r = pltpu.make_async_copy(r_hbm, rbuf, l_sem.at[2])
    own_w.start()
    ex_a.start()
    own_a.start()
    own_r.start()

    barrier = pltpu.get_barrier_semaphore()
    peers = [dev(dx=d, core=cd) for d in AROUND for cd in CORES] + [dev(core=1 - c)]
    peers += [dev(dy=1), dev(dy=3), dev(dz=1), dev(dz=2), dev(dz=3)]
    for peer in peers:
        pl.semaphore_signal(barrier, inc=1, device_id=peer, device_id_type=MESH)
    pl.semaphore_wait(barrier, len(peers))

    def cross_start(k):
        for d in AROUND:
            for cd in CORES:
                cross(k, d, cd).start()

    def bcast_start(k):
        await_bytes(abuf.at[k, y, :, pl.ds(1, 3)], a_r.at[k])
        for i in CORES:
            bcast(k, i, 0).start()
            bcast(k, 1 - i, 1).start()

    def forward_start(k):
        for back in CORES:
            bcast(k, back, back).wait_recv()
            forward(k, back).start()

    def take(part, j, zr):
        await_bytes(wview(part, j, zr), w_arrival(part, (j, zr)))
        dcopy(part, (j, zr)).start()

    def relay_x(part, j, zr):
        take(part, j, zr)
        wsend(part, (j, zr), (2, zr), dev(dx=4 - j))

    def pass_half(part, j, zr):
        wsend(2 + 2 * part + dict(SIDES)[j], (j, zr), (2, zr), dev(dx=4 - j))

    def take_halves(part, zr):
        await_bytes(wview(part, 2, zr), w_arrival(2 + 2 * part, (2, zr)))
        dcopy(part, (2, zr)).start()

    def relay_z(j, zr):
        take(1, j, zr)
        wsend(1, (j, zr), (j, 2), dev(dz=4 - zr))

    def both_x(part, zr):
        wsend(part, (0, zr), (3, zr), dev(dx=1))
        wsend(part, (0, zr), (1, zr), dev(dx=3))

    def both_z(part, j):
        wsend(part, (j, 0), (j, 3), dev(dz=1))
        wsend(part, (j, 0), (j, 1), dev(dz=3))

    partner_a = rdma(a_hbm.at[(tp + 1 - 2 * c) * 4 + z, pl.ds(0, NK)], abuf.at[:, :, c, 0],
                     p_s, p_r, dev(core=1 - c))
    own_w.wait()
    wsend(0, (0, 0), (0, 3), dev(dz=1))
    wsend(0, (0, 0), (0, 1), dev(dz=3))
    both_x(1, 0)
    cross_start(0)
    both_z(1, 0)
    wsend(0, (0, 0), (0, 2), dev(dz=2))
    cross_start(1)
    partner_a.start()
    dcopy(0, (0, 0)).start()
    dcopy(1, (0, 0)).start()

    ex_a.wait()

    def ex_copy(d, cd):
        owner = ((x + d) % 4) * 2 + cd
        return rdma(eout.at[owner], ein.at[tp], e_s, e_r, dev(dx=d, core=cd))

    def ex_product(i, carry):
        lhs = ea[pl.ds(i * 4, 4)].reshape(4 * CR, KB)
        prod = jnp.dot(lhs, wbuf[0, c, 0], preferred_element_type=F32)
        eout[i] = prod.astype(BF16).reshape(4, CR, CB)
        return carry

    lax.fori_loop(0, 8, ex_product, 0)

    take(0, 0, 3)
    take(0, 0, 1)
    wsend(0, (0, 3), (3, 3), dev(dx=1))
    wsend(0, (0, 1), (1, 1), dev(dx=3))
    wsend(0, (0, 1), (3, 1), dev(dx=1))
    wsend(0, (0, 3), (1, 3), dev(dx=3))
    bcast_start(0)
    for j, half in SIDES:
        take(1, j, 0)
        pass_half(1, j, 0)
        both_z(1, j)
    cross_start(2)
    relay_z(0, 3)
    take(1, 0, 1)
    forward_start(0)
    take(0, 0, 2)
    bcast_start(1)
    relay_x(0, 3, 3)
    relay_x(0, 1, 1)
    both_x(0, 2)
    cross_start(3)
    take(0, 3, 1)
    take(0, 1, 3)
    take_halves(1, 0)
    both_z(1, 2)
    relay_z(1, 1)
    relay_z(3, 3)
    forward_start(1)
    bcast_start(2)
    relay_z(2, 1)
    for slot in ((3, 1), (1, 3), (2, 3)):
        take(1, *slot)
    take(0, 2, 3)
    take(0, 2, 1)
    own_a.wait()
    partner_a.wait_recv()

    def partner_w(zr):
        await_bytes(wbuf.at[:, 1 - c, zr], d_r.at[zr])

    partner_w(1)
    partner_w(3)

    def tile(k, zr, out):
        for j in range(4):
            for cc in CORES:
                lhs = abuf[k, :, cc, j].reshape(CR, KB)
                term = jnp.dot(lhs, wbuf[j, cc, zr], preferred_element_type=F32).astype(BF16).astype(F32)
                if j == 0 and cc == 0:
                    out[...] = term
                else:
                    out[...] += term

    def qsend(g, n):
        view = sq.at[g, t2]
        return rdma(view, view, q_s.at[g // LAST], q_r.at[g], dev(dy=n % 4, dz=n // 4))

    def square_group(g):
        for i in (1, 0) if g == LAST else CORES:
            k = 2 * g + i
            if k < NK:
                await_bytes(yin.at[pl.ds(0, 3)], y_r.at[k])
            for q in range(4):
                hid = yin[q * NC + k] + rbuf[q, pl.ds(k * CR, CR), :].astype(F32)
                yin[q * NC + k] = hid
                hbuf[q, pl.ds(k * CR, CR), :] = hid.astype(BF16)
                total = jnp.sum(hid * hid, axis=1, keepdims=True)
                sq[g, t2, pl.ds(i * 4 + q, 1), :] = jnp.broadcast_to(total, (CR, 128)).T[0:1, :]
        for n in FAR_FIRST if g == LAST else AROUND:
            qsend(g, n).start()

    def zsend(g, dz):
        view = sz.at[g, z]
        return rdma(view, view, q_s.at[0], z_r.at[g], dev(dz=dz))

    def sum_y(g):
        await_bytes(sq.at[g, pl.ds(0, 3)], q_r.at[g])
        sz[g, z] = jnp.sum(sq[g, pl.ds(z * 4, 4)], axis=0)
        for dz in AROUND:
            zsend(g, dz).start()

    def norm_group(g):
        partial = sq if g == LAST else sz
        await_bytes(partial.at[g, pl.ds(0, 15 if g == LAST else 3)], (q_r if g == LAST else z_r).at[g])
        inv_ref[g] = lax.rsqrt(jnp.sum(partial[g], axis=0) * (1.0 / 4096) + EPS_NORM)

    def step(k, carry):
        await_bytes(abuf.at[k, pl.ds(0, 2), :, pl.ds(1, 3)], f_r.at[k])
        for zr in (1, 3):
            tile(k, zr, yout.at[k, zr - 1])
            ysend(k, zr).start()

        @pl.when(k == 0)
        def _():
            for j, half in SIDES:
                take(0, j, 2)
                pass_half(0, j, 2)
            cross_start(4)
            forward_start(2)

        @pl.when(k == 1)
        def _():
            bcast_start(3)
            for n in range(5, NK):
                cross_start(n)
            both_x(0, 0)
            await_bytes(wbuf.at[:, c, 2, pl.ds(*PARTS[1])], w_arrival(1, (0, 2)))
            for j in range(4):
                dcopy(1, (j, 2)).start()
            take_halves(0, 2)

        @pl.when(k == 2)
        def _():
            partner_w(2)

        def far(i, carry):
            tile(i, 2, yout.at[i, 1])
            ysend(i, 2).start()
            return carry

        lax.fori_loop(jnp.where(k == 2, 0, k), jnp.where(k < 2, 0, k + 1), far, 0)

        @pl.when((k >= 2) & (k < NK - 1))
        def _():
            forward_start(k + 1)

        @pl.when((k >= 2) & (k < NK - 2))
        def _():
            bcast_start(k + 2)

        @pl.when(k == 2)
        def _():
            ex_copy(0, 1 - c).start()
            for d in AROUND:
                ex_copy(d, 0).start()

        @pl.when(k == 3)
        def _():
            for j, half in SIDES:
                take(0, j, 0)
                pass_half(0, j, 0)
            for d in AROUND:
                ex_copy(d, 1).start()

        @pl.when(k == 5)
        def _():
            take_halves(0, 0)

        return carry

    own_r.wait()
    lax.fori_loop(0, NK, step, 0)
    partner_w(0)

    def near(i, carry):
        tile(i, 0, yin.at[z * NC + i])
        return carry

    lax.fori_loop(0, NK, near, 0)

    def ex_sum(q, carry):
        total = eout[tp, q].astype(F32)
        for d in range(1, 8):
            total += ein[(tp + d) % 8, q].astype(F32)
        yin[q * NC + NK] = total
        return carry

    for g in range(LAST):
        square_group(g)
    sum_y(0)
    sum_y(1)
    await_bytes(ein.at[pl.ds(0, 7)], e_r)
    lax.fori_loop(0, 4, ex_sum, 0)
    sum_y(2)
    square_group(LAST)
    for g in range(LAST + 1):
        norm_group(g)

    partner_a.wait_send()
    await_bytes(abuf.at[:, :, :, pl.ds(1, 3)], a_s)
    await_bytes(yout, y_s)
    await_bytes(yin.at[pl.ds(0, 30)], w_s)
    await_bytes(yin, d_s)
    await_bytes(eout.at[pl.ds(0, 7)], e_s)
    await_bytes(sq.at[pl.ds(0, LAST), pl.ds(0, 6)], q_s.at[0])
    await_bytes(sq.at[0, pl.ds(0, 15)], q_s.at[1])


def norm_kernel(yin, hbuf, inv_ref, g_ref, h_hbm, n_hbm, nbuf, sem):
    h_copy = pltpu.make_async_copy(hbuf, h_hbm, sem.at[0])
    h_copy.start()

    def chunk(k, carry):
        rows = pl.ds(k * CR, CR)
        for q in range(4):
            inv = inv_ref[k // 2, pl.ds((k % 2) * 4 + q, 1), :]
            scale = jnp.broadcast_to(inv, (128, CR)).T
            for half in CORES:
                cols = pl.ds(half * 128, 128)
                nbuf[q, rows, cols] = (yin[q * NC + k, :, cols] * scale * g_ref[:, cols]).astype(BF16)
        pltpu.make_async_copy(nbuf.at[:, rows], n_hbm.at[:, rows], sem.at[1]).start()
        return carry

    lax.fori_loop(0, NC, chunk, 0)
    h_copy.wait()
    pltpu.make_async_copy(nbuf, n_hbm, sem.at[1]).wait()


def solution(mesh):
    def local_step(attn_blk, w_blk, res_blk, gain_blk):
        any_spec = pl.BlockSpec(memory_space=pl.ANY)
        out = jax.ShapeDtypeStruct((4, NC * CR, CB), BF16)
        vmem_spec = pl.BlockSpec(memory_space=pltpu.VMEM)
        dma = pltpu.SemaphoreType.DMA
        hidden, h_bf16, inv = pl.pallas_call(
            kernel,
            out_shape=(pltpu.VMEM((4 * NC, CR, CB), F32), pltpu.VMEM((4, NC * CR, CB), BF16),
                       pltpu.VMEM((NC // 2, 8, 128), F32)),
            in_specs=[any_spec, any_spec, any_spec],
            out_specs=(vmem_spec,) * 3,
            scratch_shapes=[
                pltpu.VMEM((NK, 4, 2, 4, SUB, KB), BF16),
                pltpu.VMEM((4, 2, 4, KB, CB), BF16),
                pltpu.VMEM((NK, 3, CR, CB), F32),
                pltpu.VMEM((4, NC * CR, CB), BF16),
                pltpu.VMEM((NC // 2, 16, 8, 128), F32),
                pltpu.VMEM((NC // 2, 4, 8, 128), F32),
                pltpu.VMEM((32, 4, SUB, KB), BF16),
                pltpu.VMEM((8, 4, CR, CB), BF16),
                pltpu.VMEM((8, 4, CR, CB), BF16),
                dma((4,)),
                dma, dma((NK,)), dma, dma, dma((NK, 2)), dma((NK,)),
                dma, dma((27,)), dma, dma((4,)), dma, dma((NK,)),
                dma((2,)), dma((LAST + 1,)), dma, dma, dma((LAST,)),
            ],
            compiler_params=pltpu.CompilerParams(
                collective_id=0, has_side_effects=True, vmem_limit_bytes=50 * 1024 * 1024),
        )(attn_blk.reshape(8 * 4, NC, 4, SUB, KB), w_blk, res_blk.reshape(4, NC * CR, CB))
        h, n = pl.pallas_call(
            norm_kernel,
            out_shape=(out, out),
            in_specs=[vmem_spec] * 4,
            out_specs=(any_spec, any_spec),
            scratch_shapes=[pltpu.VMEM((4, NC * CR, CB), BF16), dma((2,))],
            compiler_params=pltpu.CompilerParams(vmem_limit_bytes=12 * 1024 * 1024),
        )(hidden, h_bf16, inv, gain_blk.reshape(1, CB))
        return h.reshape(4 * NC * CR, CB), n.reshape(4 * NC * CR, CB)

    row_spec = P(("dp", "tp"), "tp2")
    return jax.shard_map(local_step, mesh=mesh, in_specs=(P("dp", "tp"), P("tp", "tp2"), row_spec, P("tp2")),
                         out_specs=(row_spec, row_spec), check_vma=False)
```
